32 devices in a mesh: rep: 4 (over y, z), data: 8 (over x, core).
Axes of the slice: x: 4, y: 2, z: 2, core: 2. Of those that a mesh axis runs over, the one named last changes fastest.
The devices are a block of a 4x4x8 slice.
Arguments:
- W_in: float32 [16384, 1024], P('rep'), parts along dimension 0
- W1: float32 [4, 1024, 4096], P('rep'), parts along dimension 0
- W2: float32 [4, 4096, 1024], P('rep'), parts along dimension 0
- m_in: float32 [16384, 1024], P('rep'), parts along dimension 0
- v_in: float32 [16384, 1024], P('rep'), parts along dimension 0
- m1: float32 [4, 1024, 4096], P('rep'), parts along dimension 0
- v1: float32 [4, 1024, 4096], P('rep'), parts along dimension 0
- m2: float32 [4, 4096, 1024], P('rep'), parts along dimension 0
- v2: float32 [4, 4096, 1024], P('rep'), parts along dimension 0
- X0: bfloat16 [8192, 4096], P(('rep', 'data')), parts along dimension 0
- Y0: bfloat16 [8192, 1024], P(('rep', 'data')), parts along dimension 0
- X1: bfloat16 [8192, 4096], P(('rep', 'data')), parts along dimension 0
- Y1: bfloat16 [8192, 1024], P(('rep', 'data')), parts along dimension 0
Outputs:
- output 1: float32 [16384, 1024], P('rep'), parts along dimension 0
- output 2: float32 [4, 1024, 4096], P('rep'), parts along dimension 0
- output 3: float32 [4, 4096, 1024], P('rep'), parts along dimension 0
- output 4: float32 [16384, 1024], P('rep'), parts along dimension 0
- output 5: float32 [16384, 1024], P('rep'), parts along dimension 0
- output 6: float32 [4, 1024, 4096], P('rep'), parts along dimension 0
- output 7: float32 [4, 1024, 4096], P('rep'), parts along dimension 0
- output 8: float32 [4, 4096, 1024], P('rep'), parts along dimension 0
- output 9: float32 [4, 4096, 1024], P('rep'), parts along dimension 0
- output 10: float32 [8192], P(('rep', 'data')), parts along dimension 0
- output 11: float32 [8192, 1024], P(('rep', 'data')), parts along dimension 0
There are 4 independent parts. The reference program is written for one: setup_inputs(seed, part) draws one part's arguments, and reference() takes and returns one part's arrays. A program takes and returns all parts, laid end to end along the dimension named above; each array names one.
All inputs are finite; a program needn't handle non-finite values.
Results may differ from the reference program's by a relative error of at most 0.0174769.
Values are sent between devices in bfloat16 or wider.
A program may use at most 768 MiB of HBM per device.

```python
import jax
import jax.numpy as jnp
from jax import lax

TOK = 256
DATA = 8
L = 1
D = 1024
F = 4096
E = 4096

N = TOK * DATA
BETA1 = 0.9
BETA2 = 0.999
BC1 = 1.0 / (1.0 - BETA1 ** 10)
BC2 = 1.0 / (1.0 - BETA2 ** 10)
EPS = 1e-12
WD = 0.01
ETA = 0.05
R2 = 0.7071067811865476
R2PI = 0.3989422804014327


def gelu_grad(a):
    return 0.5 * (1.0 + lax.erf(a * R2)) + a * jnp.exp(-0.5 * a * a) * R2PI


def loss_f32(wi, w1, w2, x, y):
    def layer(h, w):
        return h + jnp.dot(jax.nn.gelu(jnp.dot(h, w[0]), approximate=False), w[1]), None
    h, _ = lax.scan(layer, jnp.dot(x, wi), (w1, w2))
    return jnp.sum((h - y) ** 2) / (2.0 * N * D)


def tokens(key, width):
    k1, k2, k3 = jax.random.split(key, 3)
    mu = jax.random.normal(k1, (DATA, 1, width), jnp.float32)
    sc = jax.random.uniform(k2, (DATA, 1, 1), jnp.float32, 0.5, 1.5)
    z = jax.random.normal(k3, (DATA, TOK, width), jnp.float32)
    return (z * sc + mu).reshape(N, width).astype(jnp.bfloat16)


def rms(g):
    return jnp.sqrt(jnp.mean(g * g, axis=(-2, -1), keepdims=True))


def moments(key, s, shape):
    ka, kb = jax.random.split(key)
    m = 0.1 * s * jax.random.normal(ka, shape, jnp.float32)
    v = 1e-3 * s * s * jax.random.uniform(kb, shape, jnp.float32, 0.5, 1.5)
    return m, v


def setup_inputs(seed: int = 0, part: int = 0) -> dict:
    ks = jax.random.split(jax.random.fold_in(jax.random.key(seed), part), 10)
    wi = jax.random.normal(ks[0], (E, D), jnp.float32) * E ** -0.5
    w1 = jax.random.normal(ks[1], (L, D, F), jnp.float32) * D ** -0.5
    w2 = jax.random.normal(ks[2], (L, F, D), jnp.float32) * (0.5 * F ** -0.5)
    x0 = tokens(ks[3], E)
    y0 = tokens(ks[4], D)
    x1 = tokens(ks[5], E)
    y1 = tokens(ks[6], D)
    gi, g1, g2 = jax.grad(loss_f32, argnums=(0, 1, 2))(wi, w1, w2, x0.astype(jnp.float32), y0.astype(jnp.float32))
    mi, vi = moments(ks[7], rms(gi), (E, D))
    m1, v1 = moments(ks[8], rms(g1), (L, D, F))
    m2, v2 = moments(ks[9], rms(g2), (L, F, D))
    return {'W_in': wi, 'W1': w1, 'W2': w2, 'm_in': mi, 'v_in': vi, 'm1': m1, 'v1': v1, 'm2': m2, 'v2': v2, 'X0': x0, 'Y0': y0, 'X1': x1, 'Y1': y1}


def forward_saved(wib, w1b, w2b, x):
    def layer(h, w):
        a = jnp.dot(h.astype(jnp.bfloat16), w[0], preferred_element_type=jnp.float32)
        s = jax.nn.gelu(a, approximate=False).astype(jnp.bfloat16)
        return h + jnp.dot(s, w[1], preferred_element_type=jnp.float32), (h, a)
    return lax.scan(layer, jnp.dot(x, wib, preferred_element_type=jnp.float32), (w1b, w2b))


def forward(wib, w1b, w2b, x):
    def layer(h, w):
        a = jnp.dot(h.astype(jnp.bfloat16), w[0], preferred_element_type=jnp.float32)
        s = jax.nn.gelu(a, approximate=False).astype(jnp.bfloat16)
        return h + jnp.dot(s, w[1], preferred_element_type=jnp.float32), None
    h, _ = lax.scan(layer, jnp.dot(x, wib, preferred_element_type=jnp.float32), (w1b, w2b))
    return h


def local_grads(wib, w1b, w2b, x, y):
    hl, (hs, acts) = forward_saved(wib, w1b, w2b, x)

    def back(g, inp):
        h, a, w1, w2 = inp
        gb = g.astype(jnp.bfloat16)
        s = jax.nn.gelu(a, approximate=False).astype(jnp.bfloat16)
        dw2 = jnp.dot(s.T, gb, preferred_element_type=jnp.float32).astype(jnp.bfloat16)
        e = (jnp.dot(gb, w2.T, preferred_element_type=jnp.float32) * gelu_grad(a)).astype(jnp.bfloat16)
        dw1 = jnp.dot(h.astype(jnp.bfloat16).T, e, preferred_element_type=jnp.float32).astype(jnp.bfloat16)
        return g + jnp.dot(e, w1.T, preferred_element_type=jnp.float32), (dw1, dw2)

    g_last = (hl - y.astype(jnp.float32)) * (1.0 / (N * D))
    g0, (dw1, dw2) = lax.scan(back, g_last, (hs, acts, w1b, w2b), reverse=True)
    dwi = jnp.dot(x.T, g0.astype(jnp.bfloat16), preferred_element_type=jnp.float32).astype(jnp.bfloat16)
    return dwi, dw1, dw2


def lamb(w, g, m, v):
    m2 = BETA1 * m + (1.0 - BETA1) * g
    v2 = BETA2 * v + (1.0 - BETA2) * g * g
    u = BC1 * m2 / (jnp.sqrt(BC2 * v2) + EPS) + WD * w
    r = jnp.sqrt(jnp.sum(w * w, axis=(-2, -1), keepdims=True)) / jnp.sqrt(jnp.sum(u * u, axis=(-2, -1), keepdims=True))
    return w - ETA * r * u, m2, v2


def reference(W_in, W1, W2, m_in, v_in, m1, v1, m2, v2, X0, Y0, X1, Y1):
    wib = W_in.astype(jnp.bfloat16)
    w1b = W1.astype(jnp.bfloat16)
    w2b = W2.astype(jnp.bfloat16)

    def acc(c, xy):
        gi, g1, g2 = local_grads(wib, w1b, w2b, xy[0], xy[1])
        return (c[0] + gi.astype(jnp.float32), c[1] + g1.astype(jnp.float32), c[2] + g2.astype(jnp.float32)), None

    zero = (jnp.zeros((E, D), jnp.float32), jnp.zeros((L, D, F), jnp.float32), jnp.zeros((L, F, D), jnp.float32))
    (gi, g1, g2), _ = lax.scan(acc, zero, (X0.reshape(DATA, TOK, E), Y0.reshape(DATA, TOK, D)))
    wi_n, mi_n, vi_n = lamb(W_in, gi.astype(jnp.bfloat16).astype(jnp.float32), m_in, v_in)
    w1_n, m1_n, v1_n = lamb(W1, g1.astype(jnp.bfloat16).astype(jnp.float32), m1, v1)
    w2_n, m2_n, v2_n = lamb(W2, g2.astype(jnp.bfloat16).astype(jnp.float32), m2, v2)
    nwi = wi_n.astype(jnp.bfloat16)
    nw1 = w1_n.astype(jnp.bfloat16)
    nw2 = w2_n.astype(jnp.bfloat16)
    h = lax.map(lambda xb: forward(nwi, nw1, nw2, xb), X1.reshape(DATA, TOK, E)).reshape(N, D)
    loss = jnp.sum((h - Y1.astype(jnp.float32)) ** 2, axis=-1) / (2.0 * D)
    return (wi_n, w1_n, w2_n, mi_n, vi_n, m1_n, v1_n, m2_n, v2_n, loss, h)
```

```python
import functools

import jax
import jax.numpy as jnp
from jax import lax
from jax.experimental import pallas as pl
from jax.experimental.pallas import tpu as pltpu
from jax.sharding import PartitionSpec as P

BETA1 = 0.9
BETA2 = 0.999
BC1 = 1.0 / (1.0 - BETA1 ** 10)
BC2 = 1.0 / (1.0 - BETA2 ** 10)
EPS = 1e-12
WD = 0.01
ETA = 0.05
R2 = 0.7071067811865476
R2PI = 0.3989422804014327
BF = jnp.bfloat16
F32 = jnp.float32


def gelu(a):
    return 0.5 * a * (1.0 + lax.erf(a * R2))


def gelu_grad(a):
    return 0.5 * (1.0 + lax.erf(a * R2)) + a * jnp.exp(-0.5 * a * a) * R2PI


MESH = pl.DeviceIdType.MESH
ROUNDS = 6


def fold8(x):
    return jnp.sum(x.reshape(x.shape[0] // 8, 8, x.shape[1]), axis=0)


def moments(w, g, m, v):
    m2 = BETA1 * m + (1.0 - BETA1) * g
    v2 = BETA2 * v + (1.0 - BETA2) * g * g
    u = BC1 * m2 / (jnp.sqrt(BC2 * v2) + EPS) + WD * w
    return m2, v2, u


def sum_kernel(p, s_ref, gb_ref, hb_ref, a_ref, g_ref, x_ref, w2, m2, v2, w1, m1, v1, wi, mi, vi,
               o2, o1, oi, cs_ref,
               st, pr, pt, rb, e_s, h_t, g0_s, wa, wb, lw, gst, ns, nr,
               d_send, d_recv, r_send, r_recv, credit, pcredit, w_sem, l_sem, o_sem, n_send, n_recv):
    me = lax.axis_index('data')
    core = lax.rem(me, 2)
    chip = lax.div(me, 2)
    nc = p // 2
    partner = me + 1 - 2 * core
    right = lax.rem(me + 2, p)
    left = lax.rem(me + p - 2, p)
    dims_t = (((1,), (1,)), ((), ()))

    def owner(t, k):
        return 2 * lax.rem(chip + t, nc) + k

    def remote(src, dst, ss, rs, dev):
        return pltpu.make_async_remote_copy(src_ref=src, dst_ref=dst, send_sem=ss, recv_sem=rs,
                                            device_id={'data': dev}, device_id_type=MESH)

    def d2d(b, t):
        return remote(st.at[b, t], pr.at[b, t], d_send.at[b, t], d_recv.at[b, t], partner)

    up, lo = pl.ds(0, 128), pl.ds(128, 128)
    routes = ((2, up, 0, right), (2, lo, 1, left), (1, lo, 2, right), (3, up, 3, left), (1, up, 4, right), (3, lo, 5, left))

    def ring(b, n):
        t, half, slot, dev = routes[n]
        return remote(pt.at[b, t, half], rb.at[b, slot], r_send.at[b, n], r_recv.at[b, n], dev)

    def tile(r, j, store):
        h = r % 2
        if r // 2 == 1:
            rows = pl.ds(pl.multiple_of(j * 128 + h * 64, 64), 64)
            for q in range(4):
                d = jnp.dot(h_t[rows, :], e_s[:, q * 1024:(q + 1) * 1024], preferred_element_type=F32)
                store(pl.ds(q * 64, 64), d.astype(BF))
        else:
            x, y = (s_ref, gb_ref) if r < 2 else (x_ref, g0_s)
            cols = pl.ds(pl.multiple_of(j * 512 + h * 256, 256), 256)
            d = jnp.dot(x[:, cols].T, y[...], preferred_element_type=F32)
            store(pl.ds(0, 256), d.astype(BF))

    def s1(r):
        b = r % 2
        if r >= 2:
            pl.semaphore_wait(pcredit, 1)

        def theirs(t, _):
            def put(rows, d):
                st[b, t, rows] = d
            tile(r, owner(t, 1 - core), put)

            @pl.when(t > 0)
            def _():
                d2d(b, t - 1).start()
            return 0

        lax.fori_loop(0, nc, theirs, 0)

        def ours(t, _):
            def put(rows, d):
                pt[b, t, rows] = d.astype(F32)
            tile(r, owner(t, core), put)

            @pl.when(t == 0)
            def _():
                d2d(b, nc - 1).start()
            return 0

        lax.fori_loop(0, nc, ours, 0)

    def s2(r):
        b = r % 2
        if r >= 2:
            pl.semaphore_wait(credit.at[0], 1)
            pl.semaphore_wait(credit.at[1], 1)
        for t in (2, 1, 3, 0):
            d2d(b, t).wait_recv()
            pt[b, t] += pr[b, t].astype(F32)
            if t == 2:
                ring(b, 0).start()
                ring(b, 1).start()
            elif t == 1:
                ring(b, 2).start()
            elif t == 3:
                ring(b, 3).start()
        for t in range(nc):
            d2d(b, t).wait_send()
        if r + 2 < ROUNDS:
            pl.semaphore_signal(pcredit, inc=1, device_id={'data': partner}, device_id_type=MESH)

    def s3(r):
        b = r % 2
        ring(b, 0).wait_recv()
        pt[b, 1, up] += rb[b, 0]
        ring(b, 4).start()
        ring(b, 1).wait_recv()
        pt[b, 3, lo] += rb[b, 1]
        ring(b, 5).start()

    def shard_loads(r):
        k, h = r // 2, r % 2
        out = []
        for n, ref in enumerate(((w2, m2, v2), (w1, m1, v1), (wi, mi, vi))[k]):
            if k == 1:
                for q in range(4):
                    rows = pl.ds(pl.multiple_of(me * 128 + h * 64, 64), 64)
                    out.append(pltpu.make_async_copy(ref.at[rows, pl.ds(q * 1024, 1024)],
                                                     lw.at[n, pl.ds(q * 64, 64)], l_sem.at[n, q]))
            else:
                rows = pl.ds(pl.multiple_of(me * 512 + h * 256, 256), 256)
                out.append(pltpu.make_async_copy(ref.at[rows], lw.at[n], l_sem.at[n, 0]))
        return out

    def put_out(r):
        k, h = r // 2, r % 2
        rows = pl.ds(h * 256, 256)
        return pltpu.make_async_copy(gst.at[k, rows], (o2, o1, oi)[k].at[rows], o_sem.at[k, h])

    def s4(r):
        b, k, h = r % 2, r // 2, r % 2
        loads = shard_loads(r)
        for c in loads:
            c.start()
        for n in (2, 3, 4, 5):
            ring(b, n).wait_recv()
        gst[k, pl.ds(h * 256, 128)] = (pt[b, 0, up] + rb[b, 4] + rb[b, 3]).astype(BF)
        gst[k, pl.ds(h * 256 + 128, 128)] = (pt[b, 0, lo] + rb[b, 5] + rb[b, 2]).astype(BF)
        for n in range(6):
            ring(b, n).wait_send()
        if r + 2 < ROUNDS:
            pl.semaphore_signal(credit.at[0], inc=1, device_id={'data': right}, device_id_type=MESH)
            pl.semaphore_signal(credit.at[1], inc=1, device_id={'data': left}, device_id_type=MESH)
        for c in loads:
            c.wait()
        put_out(r).start()
        sw = jnp.zeros((8, 1024), F32)
        su = jnp.zeros((8, 1024), F32)
        for i in range(4):
            rows = pl.ds(i * 64, 64)
            w = lw[0, rows]
            _, _, u = moments(w, gst[k, pl.ds(h * 256 + i * 64, 64)].astype(F32), lw[1, rows], lw[2, rows])
            sw += fold8(w * w)
            su += fold8(u * u)
        for n, t in enumerate((sw, su)):
            f = t[:, 0:128]
            for q in range(1, 8):
                f += t[:, q * 128:(q + 1) * 128]
            row = pl.ds((2 * k + n) * 8, 8)
            if h == 0:
                ns[row] = f
            else:
                ns[row] += f

    def load_a(i):
        return pltpu.make_async_copy(w2.at[pl.ds(i * 256, 256)], wa.at[lax.rem(i, 2)], w_sem.at[lax.rem(i, 2)])

    def load_b(i):
        return pltpu.make_async_copy(w1.at[pl.ds(i * 128, 128)], wb.at[lax.rem(i, 2)], w_sem.at[lax.rem(i, 2)])

    def make_e():
        n = s_ref.shape[1] // 256
        load_a(0).start()
        h_t[...] = hb_ref[...].T

        def body(i, _):
            @pl.when(i + 1 < n)
            def _():
                load_a(i + 1).start()
            load_a(i).wait()
            cols = pl.ds(pl.multiple_of(i * 256, 256), 256)
            d = lax.dot_general(gb_ref[...], wa[lax.rem(i, 2)].astype(BF), dims_t, preferred_element_type=F32)
            e_s[:, cols] = (d * gelu_grad(a_ref[:, cols])).astype(BF)
            return 0

        lax.fori_loop(0, n, body, 0)

    def make_g0():
        n = gb_ref.shape[1] // 128
        load_b(0).start()

        def body(i, _):
            @pl.when(i + 1 < n)
            def _():
                load_b(i + 1).start()
            load_b(i).wait()
            cols = pl.ds(pl.multiple_of(i * 128, 128), 128)
            d = lax.dot_general(e_s[...], wb[lax.rem(i, 2)].astype(BF), dims_t, preferred_element_type=F32)
            g0_s[:, cols] = (g_ref[:, cols] + d).astype(BF)
            return 0

        lax.fori_loop(0, n, body, 0)

    barrier = pltpu.get_barrier_semaphore()
    for o in range(1, p):
        pl.semaphore_signal(barrier, inc=1, device_id={'data': lax.rem(me + o, p)}, device_id_type=MESH)
    pl.semaphore_wait(barrier, p - 1)

    s1(0)
    s2(0)
    for r in range(ROUNDS):
        if r + 1 < ROUNDS:
            s1(r + 1)
        s3(r)
        if r + 1 < ROUNDS:
            s2(r + 1)
        if r == 0:
            make_e()
        if r == 2:
            make_g0()
        s4(r)

    def norm(o):
        return remote(ns, nr.at[me], n_send.at[o - 1], n_recv.at[o - 1], lax.rem(me + o, p))

    nr[me] = ns[...]
    for o in range(1, p):
        norm(o).start()
    for o in range(1, p):
        norm(o).wait()
    tot = nr[0]
    for o in range(1, p):
        tot = tot + nr[o]
    for k in range(3):
        nw = jnp.sqrt(jnp.sum(tot[16 * k:16 * k + 8], keepdims=True))
        nu = jnp.sqrt(jnp.sum(tot[16 * k + 8:16 * k + 16], keepdims=True))
        cs_ref[k] = jnp.broadcast_to(ETA * (nw / nu), (8, 128))
    for r in range(ROUNDS):
        put_out(r).wait()


def reduce_grads(p, s, gb, hb, a, g, x, w2, m2, v2, w1, m1, v1, wi, mi, vi):
    vm = pl.BlockSpec(memory_space=pltpu.VMEM)
    hbm = pl.BlockSpec(memory_space=pl.ANY)
    dma, reg = pltpu.SemaphoreType.DMA, pltpu.SemaphoreType.REGULAR
    o = jax.ShapeDtypeStruct((512, 1024), BF)
    tok = x.shape[0]
    return pl.pallas_call(
        functools.partial(sum_kernel, p),
        name='sum_grads',
        in_specs=[vm] * 6 + [hbm] * 9,
        out_specs=[hbm] * 3 + [vm],
        out_shape=[o, o, o, jax.ShapeDtypeStruct((3, 8, 128), F32)],
        scratch_shapes=[
            pltpu.VMEM((2, 4, 256, 1024), BF), pltpu.VMEM((2, 4, 256, 1024), BF), pltpu.VMEM((2, 4, 256, 1024), F32),
            pltpu.VMEM((2, 6, 128, 1024), F32), pltpu.VMEM((tok, 4096), BF), pltpu.VMEM((1024, tok), BF),
            pltpu.VMEM((tok, 1024), BF), pltpu.VMEM((2, 256, 1024), F32), pltpu.VMEM((2, 128, 4096), F32),
            pltpu.VMEM((3, 256, 1024), F32), pltpu.VMEM((3, 512, 1024), BF), pltpu.VMEM((48, 128), F32), pltpu.VMEM((p, 48, 128), F32),
            dma((2, 4)), dma((2, 4)), dma((2, 6)), dma((2, 6)), reg((2,)), reg, dma((2,)), dma((3, 4)), dma((3, 2)),
            dma((p - 1,)), dma((p - 1,)),
        ],
        compiler_params=pltpu.CompilerParams(collective_id=0, has_side_effects=True, vmem_limit_bytes=60 * 2 ** 20),
        cost_estimate=pl.CostEstimate(flops=10 ** 11, bytes_accessed=10 ** 8, transcendentals=0),
    )(s, gb, hb, a, g, x, w2, m2, v2, w1, m1, v1, wi, mi, vi)


def lamb_kernel(kind, *refs):
    w_ref, m_ref, v_ref, g_ref, c_ref, x_ref = refs[:6]
    h_ref = refs[6] if kind == 'out' else None
    wo_ref, mo_ref, vo_ref, o_ref = refs[-4:]
    w = w_ref[...]
    g = g_ref[...].reshape(w.shape).astype(F32)
    m2, v2, u = moments(w, g, m_ref[...], v_ref[...])
    mo_ref[...] = m2
    vo_ref[...] = v2
    wn = w - c_ref[0:1, 0:1] * u
    wo_ref[...] = wn
    d = jnp.dot(x_ref[...], wn.astype(BF), preferred_element_type=F32)
    if kind == 'cols':
        o_ref[...] = gelu(d).astype(BF)
    else:
        j = pl.program_id(0)

        @pl.when(j == 0)
        def _():
            o_ref[...] = d if kind == 'in' else h_ref[...] + d

        @pl.when(j > 0)
        def _():
            o_ref[...] += d


def lamb(kind, w, m, v, g, c, x, h=None):
    rows, cols = w.shape
    tok = x.shape[0]
    whole = lambda s: pl.BlockSpec(s, lambda i: (0,) * len(s))
    if kind == 'cols':
        nb = cols // 256
        blk = pl.BlockSpec((rows, 256), lambda i: (0, i))
        q = g.shape[-1] // 256
        g_spec = pl.BlockSpec(g.shape[:2] + (None, g.shape[3], 256), lambda i: (0, 0, i // q, 0, i % q))
        x_spec = whole((tok, rows))
        o_spec = pl.BlockSpec((tok, 256), lambda i: (0, i))
        o_shape = jax.ShapeDtypeStruct((tok, cols), BF)
    else:
        nb = rows // 256
        blk = pl.BlockSpec((256, cols), lambda i: (i, 0))
        g_spec = blk
        x_spec = pl.BlockSpec((tok, 256), lambda i: (0, i))
        o_spec = whole((tok, cols))
        o_shape = jax.ShapeDtypeStruct((tok, cols), F32)
    ins = [w, m, v, g, c, x]
    specs = [blk] * 3 + [g_spec, whole((8, 128)), x_spec]
    if h is not None:
        ins.append(h)
        specs.append(whole((tok, cols)))
    f = jax.ShapeDtypeStruct((rows, cols), F32)
    return pl.pallas_call(
        functools.partial(lamb_kernel, kind),
        name='lamb_' + kind,
        grid=(nb,),
        in_specs=specs,
        out_specs=[blk, blk, blk, o_spec],
        out_shape=[f, f, f, o_shape],
        compiler_params=pltpu.CompilerParams(dimension_semantics=('arbitrary',), vmem_limit_bytes=40 * 2 ** 20),
        cost_estimate=pl.CostEstimate(flops=30 * 10 ** 9, bytes_accessed=rows * cols * 26, transcendentals=0),
    )(*ins)


def solution(mesh):
    p = mesh.shape['data']

    def gather(s):
        return lax.all_gather(s, 'data', axis=0, tiled=True)

    def step(wi, w1, w2, mi, vi, m1, v1, m2, v2, x0, y0, x1, y1):
        w1, w2, m1, v1, m2, v2 = (t[0] for t in (w1, w2, m1, v1, m2, v2))
        d = wi.shape[1]
        scale = 1.0 / (x0.shape[0] * p * d)
        h = jnp.dot(x0, wi.astype(BF), preferred_element_type=F32)
        hb = h.astype(BF)
        a = jnp.dot(hb, w1.astype(BF), preferred_element_type=F32)
        s = gelu(a).astype(BF)
        h = h + jnp.dot(s, w2.astype(BF), preferred_element_type=F32)
        g = (h - y0.astype(F32)) * scale
        s2, s1, si, c = reduce_grads(p, s, g.astype(BF), hb, a, g, x0, w2, m2, v2, w1, m1, v1, wi, mi, vi)
        gi = gather(si)
        g1 = gather(s1).reshape(p, 2, 4, 64, 1024)
        g2 = gather(s2)
        wi_n, mi_n, vi_n, h = lamb('in', wi, mi, vi, gi, c[2], x1)
        w1_n, m1_n, v1_n, s = lamb('cols', w1, m1, v1, g1, c[1], h.astype(BF))
        w2_n, m2_n, v2_n, h = lamb('out', w2, m2, v2, g2, c[0], s, h)
        loss = jnp.sum((h - y1.astype(F32)) ** 2, axis=-1) / (2.0 * d)
        return (wi_n, w1_n[None], w2_n[None], mi_n, vi_n, m1_n[None], v1_n[None], m2_n[None], v2_n[None], loss, h)

    w2s = P('rep', None)
    w3s = P('rep', None, None)
    ts = P(('rep', 'data'), None)
    return jax.shard_map(step, mesh=mesh,
                         in_specs=(w2s, w3s, w3s, w2s, w2s, w3s, w3s, w3s, w3s, ts, ts, ts, ts),
                         out_specs=(w2s, w3s, w3s, w2s, w2s, w3s, w3s, w3s, w3s, P(('rep', 'data')), ts),
                         check_vma=False)
```

```python
import functools

import jax
import jax.numpy as jnp
from jax import lax
from jax.experimental import pallas as pl
from jax.experimental.pallas import tpu as pltpu
from jax.sharding import PartitionSpec as P

BETA1 = 0.9
BETA2 = 0.999
BC1 = 1.0 / (1.0 - BETA1 ** 10)
BC2 = 1.0 / (1.0 - BETA2 ** 10)
EPS = 1e-12
WD = 0.01
ETA = 0.05
R2 = 0.7071067811865476
R2PI = 0.3989422804014327
BF = jnp.bfloat16
F32 = jnp.float32


def gelu(a):
    return 0.5 * a * (1.0 + lax.erf(a * R2))


def gelu_grad(a):
    return 0.5 * (1.0 + lax.erf(a * R2)) + a * jnp.exp(-0.5 * a * a) * R2PI


MESH = pl.DeviceIdType.MESH
ROUNDS = 6


def fold8(x):
    return jnp.sum(x.reshape(x.shape[0] // 8, 8, x.shape[1]), axis=0)


def moments(w, g, m, v):
    m2 = BETA1 * m + (1.0 - BETA1) * g
    v2 = BETA2 * v + (1.0 - BETA2) * g * g
    u = BC1 * m2 / (jnp.sqrt(BC2 * v2) + EPS) + WD * w
    return m2, v2, u


def sum_kernel(p, x_ref, y_ref, w2, m2, v2, w1, m1, v1, wi, mi, vi,
               o2, o1, oi, cs_ref,
               s_ref, gb_ref, hb_ref, a_ref, g_ref, st, pr, pt, rb, e_s, h_t, g0_s, wa, wb, lw, gst, ns, nr,
               d_send, d_recv, r_send, r_recv, credit, pcredit, w_sem, l_sem, o_sem, n_send, n_recv, a_send, a_recv, b_send, b_recv, f_sem):
    me = lax.axis_index('data')
    core = lax.rem(me, 2)
    chip = lax.div(me, 2)
    nc = p // 2
    partner = me + 1 - 2 * core
    right = lax.rem(me + 2, p)
    left = lax.rem(me + p - 2, p)
    dims_t = (((1,), (1,)), ((), ()))

    def owner(t, k):
        return 2 * lax.rem(chip + t, nc) + k

    def remote(src, dst, ss, rs, dev):
        return pltpu.make_async_remote_copy(src_ref=src, dst_ref=dst, send_sem=ss, recv_sem=rs,
                                            device_id={'data': dev}, device_id_type=MESH)

    def d2d(b, t):
        return remote(st.at[b, t], pr.at[b, t], d_send.at[b, t], d_recv.at[b, t], partner)

    up, lo = pl.ds(0, 128), pl.ds(128, 128)
    routes = ((2, up, 0, right), (2, lo, 1, left), (1, lo, 2, right), (3, up, 3, left), (1, up, 4, right), (3, lo, 5, left))

    def ring(b, n):
        t, half, slot, dev = routes[n]
        return remote(pt.at[b, t, half], rb.at[b, slot], r_send.at[b, n], r_recv.at[b, n], dev)

    def tile(r, j, store):
        h = r % 2
        if r // 2 == 2:
            cols = pl.ds(pl.multiple_of(j * 512 + h * 256, 256), 256)
            for q in range(4):
                d = jnp.dot(h_t[q * 256:(q + 1) * 256, :], e_s[:, cols], preferred_element_type=F32)
                store(pl.ds(q * 256, 256), d.astype(BF))
        else:
            x, y = (s_ref, gb_ref) if r < 2 else (x_ref, g0_s)
            cols = pl.ds(pl.multiple_of(j * 512 + h * 256, 256), 256)
            d = jnp.dot(x[:, cols].T, y[...], preferred_element_type=F32)
            store(pl.ds(0, 1024), d.astype(BF))

    def s1(r):
        b = r % 2
        if r >= 2:
            pl.semaphore_wait(pcredit, 1)

        def theirs(i, _):
            t = lax.rem(i + 2, nc)

            def put(cols, d):
                st[b, t, :, cols] = d
            tile(r, owner(t, 1 - core), put)

            @pl.when(i > 0)
            def _():
                d2d(b, lax.rem(i + 1, nc)).start()
            return 0

        lax.fori_loop(0, nc, theirs, 0)

        def ours(i, _):
            t = lax.rem(i + 2, nc)

            def put(cols, d):
                pt[b, t, :, cols] = d.astype(F32)
            tile(r, owner(t, core), put)

            @pl.when(i == 0)
            def _():
                d2d(b, 1).start()
            return 0

        lax.fori_loop(0, nc, ours, 0)

    def s2(r):
        b = r % 2
        if r >= 2:
            pl.semaphore_wait(credit.at[0], 1)
            pl.semaphore_wait(credit.at[1], 1)
        for t in (2, 3, 1, 0):
            d2d(b, t).wait_recv()
            pt[b, t] += pr[b, t].astype(F32)
            if t == 2:
                ring(b, 0).start()
                ring(b, 1).start()
            elif t == 1:
                ring(b, 2).start()
            elif t == 3:
                ring(b, 3).start()
        for t in range(nc):
            d2d(b, t).wait_send()
        if r + 2 < ROUNDS:
            pl.semaphore_signal(pcredit, inc=1, device_id={'data': partner}, device_id_type=MESH)

    def s3(r):
        b = r % 2
        ring(b, 0).wait_recv()
        pt[b, 1, up] += rb[b, 0]
        ring(b, 4).start()
        ring(b, 1).wait_recv()
        pt[b, 3, lo] += rb[b, 1]
        ring(b, 5).start()

    def shard_loads(r):
        k, h = r // 2, r % 2
        out = []
        at = pl.ds(pl.multiple_of(me * 512 + h * 256, 256), 256)
        for n, ref in enumerate(((w2, m2, v2), (wi, mi, vi), (w1, m1, v1))[k]):
            if k == 2:
                for q in range(4):
                    part = pl.ds(q * 256, 256)
                    out.append(pltpu.make_async_copy(ref.at[part, at], lw.at[n, :, part], l_sem.at[n, q]))
            else:
                out.append(pltpu.make_async_copy(ref.at[at], lw.at[n], l_sem.at[n, 0]))
        return out

    def put_out(r):
        k, h = r // 2, r % 2
        rows = pl.ds(h * 256, 256)
        dst = oi.at[block(me, h)] if k == 1 else (o2, oi, o1)[k].at[rows]
        return pltpu.make_async_copy(gst.at[k, rows], dst, o_sem.at[k, h])

    def block(j, h):
        return pl.ds(pl.multiple_of(j * 512 + h * 256, 256), 256)

    def ag(n):
        h = n % 2
        if n < 4:
            src, j, dev = gst.at[1, pl.ds(h * 256, 256)], me, (right, left)[n // 2]
        else:
            j, dev = (left, right)[h], (right, left)[h]
            src = oi.at[block(j, h)]
        return remote(src, oi.at[block(j, h)], a_send.at[n], a_recv.at[n], dev)

    def ag_pair(n):
        h = n % 2
        j = (me, left, right, lax.rem(me + 4, p))[n // 2]
        src = gst.at[1, pl.ds(h * 256, 256)] if n < 2 else oi.at[block(j, h)]
        return remote(src, oi.at[block(j, h)], b_send.at[n], b_recv.at[n], partner)

    def ag_own(h):
        ag(h).start()
        ag(2 + h).start()
        ag_pair(h).start()

    def ag_near(h):
        ag(h).wait_recv()
        if h == 0:
            ag(4).start()
        ag(2 + h).wait_recv()
        if h == 1:
            ag(5).start()
        ag_pair(2 + h).start()
        ag_pair(4 + h).start()

    def ag_far(h):
        ag(4 + h).wait_recv()
        ag_pair(6 + h).start()

    def s4(r):
        b, k, h = r % 2, r // 2, r % 2
        loads = shard_loads(r)
        for c in loads:
            c.start()
        for n in (2, 3, 4, 5):
            ring(b, n).wait_recv()
        gst[k, pl.ds(h * 256, 128)] = (pt[b, 0, up] + rb[b, 4] + rb[b, 3]).astype(BF)
        gst[k, pl.ds(h * 256 + 128, 128)] = (pt[b, 0, lo] + rb[b, 5] + rb[b, 2]).astype(BF)
        for n in range(6):
            ring(b, n).wait_send()
        if r + 2 < ROUNDS:
            pl.semaphore_signal(credit.at[0], inc=1, device_id={'data': right}, device_id_type=MESH)
            pl.semaphore_signal(credit.at[1], inc=1, device_id={'data': left}, device_id_type=MESH)
        for c in loads:
            c.wait()
        put_out(r).start()
        sw = jnp.zeros((8, 1024), F32)
        su = jnp.zeros((8, 1024), F32)
        for i in range(4):
            rows = pl.ds(i * 64, 64)
            w = lw[0, rows]
            _, _, u = moments(w, gst[k, pl.ds(h * 256 + i * 64, 64)].astype(F32), lw[1, rows], lw[2, rows])
            sw += fold8(w * w)
            su += fold8(u * u)
        for n, t in enumerate((sw, su)):
            f = t[:, 0:128]
            for q in range(1, 8):
                f += t[:, q * 128:(q + 1) * 128]
            row = pl.ds((2 * k + n) * 8, 8)
            if h == 0:
                ns[row] = f
            else:
                ns[row] += f

    def load_a(i):
        return pltpu.make_async_copy(w2.at[pl.ds(i * 256, 256)], wa.at[lax.rem(i, 2)], w_sem.at[lax.rem(i, 2)])

    def load_b(i):
        return pltpu.make_async_copy(w1.at[pl.ds(i * 128, 128)], wb.at[lax.rem(i, 2)], w_sem.at[lax.rem(i, 2)])

    def make_e():
        n = s_ref.shape[1] // 256
        load_a(0).start()
        h_t[...] = hb_ref[...].T

        def body(i, _):
            @pl.when(i + 1 < n)
            def _():
                load_a(i + 1).start()
            load_a(i).wait()
            cols = pl.ds(pl.multiple_of(i * 256, 256), 256)
            d = lax.dot_general(gb_ref[...], wa[lax.rem(i, 2)].astype(BF), dims_t, preferred_element_type=F32)
            e_s[:, cols] = (d * gelu_grad(a_ref[:, cols])).astype(BF)
            return 0

        lax.fori_loop(0, n, body, 0)

    def make_g0():
        n = gb_ref.shape[1] // 128
        load_b(0).start()

        def body(i, _):
            @pl.when(i + 1 < n)
            def _():
                load_b(i + 1).start()
            load_b(i).wait()
            cols = pl.ds(pl.multiple_of(i * 128, 128), 128)
            d = lax.dot_general(e_s[...], wb[lax.rem(i, 2)].astype(BF), dims_t, preferred_element_type=F32)
            g0_s[:, cols] = (g_ref[:, cols] + d).astype(BF)
            return 0

        lax.fori_loop(0, n, body, 0)

    def f_buf(u):
        return pt.at[lax.div(u, 2), pl.ds(2 * lax.rem(u, 2), 2)]

    def f_copy(src, u, n):
        return pltpu.make_async_copy(src, pt.at[lax.div(u, 2), 2 * lax.rem(u, 2) + n], f_sem.at[u, n])

    def f_start(i):
        u = lax.rem(i, 4)
        k, o = lax.div(i, 8), lax.rem(i, 8)
        for n in range(2):
            rows = pl.ds(pl.multiple_of(o * 512 + n * 256, 256), 256)

            @pl.when(k == 0)
            def _():
                f_copy(wi.at[rows], u, n).start()

            @pl.when(k == 1)
            def _():
                part = pl.ds(pl.multiple_of(lax.rem(o, 2) * 512 + n * 256, 256), 256)
                f_copy(w1.at[part, pl.ds(pl.multiple_of(lax.div(o, 2) * 1024, 1024), 1024)], u, n).start()

            @pl.when(k == 2)
            def _():
                f_copy(w2.at[rows], u, n).start()

    def f_take(i):
        u = lax.rem(i, 4)
        for n in range(2):
            f_copy(wi.at[pl.ds(0, 256)], u, n).wait()
        return f_buf(u)[...].reshape(512, 1024).astype(BF)

    def f_loop(k, body):
        def one(n, _):
            i = 8 * k + n
            body(n, f_take(i))

            @pl.when(i + 4 < 24)
            def _():
                f_start(i + 4)
            return 0

        lax.fori_loop(0, 8, one, 0)

    def chunk(n):
        return pl.ds(pl.multiple_of(n * 512, 512), 512)

    def f_in(n, w):
        d = jnp.dot(x_ref[:, chunk(n)], w, preferred_element_type=F32)

        @pl.when(n == 0)
        def _():
            g_ref[...] = d

        @pl.when(n > 0)
        def _():
            g_ref[...] += d

    def f_mid(n, w):
        cols = pl.ds(pl.multiple_of(lax.div(n, 2) * 1024, 1024), 1024)

        @pl.when(lax.rem(n, 2) == 0)
        def _():
            a_ref[:, cols] = jnp.dot(hb_ref[:, 0:512], w, preferred_element_type=F32)

        @pl.when(lax.rem(n, 2) == 1)
        def _():
            a_ref[:, cols] += jnp.dot(hb_ref[:, 512:1024], w, preferred_element_type=F32)

            def act(q, _):
                part = pl.ds(pl.multiple_of(lax.div(n, 2) * 1024 + q * 256, 256), 256)
                s_ref[:, part] = gelu(a_ref[:, part]).astype(BF)
                return 0

            lax.fori_loop(0, 4, act, 0)

    def f_out(n, w):
        g_ref[...] += jnp.dot(s_ref[:, chunk(n)], w, preferred_element_type=F32)

    barrier = pltpu.get_barrier_semaphore()
    for o in range(1, p):
        pl.semaphore_signal(barrier, inc=1, device_id={'data': lax.rem(me + o, p)}, device_id_type=MESH)
    for i in range(4):
        f_start(jnp.int32(i))
    f_loop(0, f_in)
    hb_ref[...] = g_ref[...].astype(BF)
    f_loop(1, f_mid)
    f_loop(2, f_out)
    scale = 1.0 / (x_ref.shape[0] * p * g_ref.shape[1])
    g_ref[...] = (g_ref[...] - y_ref[...].astype(F32)) * scale
    gb_ref[...] = g_ref[...].astype(BF)
    pl.semaphore_wait(barrier, p - 1)

    s1(0)
    s2(0)
    for r in range(ROUNDS):
        if r + 1 < ROUNDS:
            s1(r + 1)
        s3(r)
        if r + 1 < ROUNDS:
            s2(r + 1)
        if r == 0:
            make_e()
            make_g0()
        if r == 3:
            ag_near(0)
        if r == 4:
            ag_near(1)
            ag_far(0)
        if r == 5:
            ag_far(1)
        s4(r)
        if r // 2 == 1:
            ag_own(r % 2)

    def norm(o):
        return remote(ns, nr.at[me], n_send.at[o - 1], n_recv.at[o - 1], lax.rem(me + o, p))

    nr[me] = ns[...]
    for o in range(1, p):
        norm(o).start()
    for o in range(1, p):
        norm(o).wait()
    tot = nr[0]
    for o in range(1, p):
        tot = tot + nr[o]
    for k in range(3):
        nw = jnp.sqrt(jnp.sum(tot[16 * k:16 * k + 8], keepdims=True))
        nu = jnp.sqrt(jnp.sum(tot[16 * k + 8:16 * k + 16], keepdims=True))
        cs_ref[k] = jnp.broadcast_to(ETA * (nw / nu), (8, 128))
    for r in range(ROUNDS):
        put_out(r).wait()
    for n in range(6):
        ag(n).wait_send()
    for n in range(8):
        ag_pair(n).wait()


def reduce_grads(p, x, y, w2, m2, v2, w1, m1, v1, wi, mi, vi):
    vm = pl.BlockSpec(memory_space=pltpu.VMEM)
    hbm = pl.BlockSpec(memory_space=pltpu.HBM)
    dma, reg = pltpu.SemaphoreType.DMA, pltpu.SemaphoreType.REGULAR
    o = jax.ShapeDtypeStruct((512, 1024), BF)
    tok = x.shape[0]
    return pl.pallas_call(
        functools.partial(sum_kernel, p),
        name='sum_grads',
        in_specs=[vm] * 2 + [hbm] * 9,
        out_specs=[hbm] * 3 + [vm],
        out_shape=[o, o, jax.ShapeDtypeStruct((512 * p, 1024), BF), jax.ShapeDtypeStruct((3, 8, 128), F32)],
        scratch_shapes=[
            pltpu.VMEM((tok, 4096), BF), pltpu.VMEM((tok, 1024), BF), pltpu.VMEM((tok, 1024), BF),
            pltpu.VMEM((tok, 4096), F32), pltpu.VMEM((tok, 1024), F32),
            pltpu.VMEM((2, 4, 256, 1024), BF), pltpu.VMEM((2, 4, 256, 1024), BF), pltpu.VMEM((2, 4, 256, 1024), F32),
            pltpu.VMEM((2, 6, 128, 1024), F32), pltpu.VMEM((tok, 4096), BF), pltpu.VMEM((1024, tok), BF),
            pltpu.VMEM((tok, 1024), BF), pltpu.VMEM((2, 256, 1024), F32), pltpu.VMEM((2, 128, 4096), F32),
            pltpu.VMEM((3, 256, 1024), F32), pltpu.VMEM((3, 512, 1024), BF), pltpu.VMEM((48, 128), F32), pltpu.VMEM((p, 48, 128), F32),
            dma((2, 4)), dma((2, 4)), dma((2, 6)), dma((2, 6)), reg((2,)), reg, dma((2,)), dma((3, 4)), dma((3, 2)),
            dma((p - 1,)), dma((p - 1,)), dma((6,)), dma((6,)), dma((8,)), dma((8,)), dma((4, 2)),
        ],
        compiler_params=pltpu.CompilerParams(collective_id=0, has_side_effects=True, vmem_limit_bytes=60 * 2 ** 20),
        cost_estimate=pl.CostEstimate(flops=10 ** 11, bytes_accessed=10 ** 8, transcendentals=0),
    )(x, y, w2, m2, v2, w1, m1, v1, wi, mi, vi)


def lamb_kernel(kind, nb, has_h, w, m, v, g, c_ref, x_ref, *refs):
    h_ref = refs[0] if has_h else None
    wo, mo, vo, o_ref, ib, gb, ob, i_sem, o_sem = refs[has_h:]
    nbuf = ib.shape[0]
    size = gb.shape[1] if kind != 'cols' else ib.shape[3]

    def at(i):
        s = pl.ds(pl.multiple_of(i * size, size), size)
        return (slice(None), s) if kind == 'cols' else (s, slice(None))

    def loads(i):
        b = lax.rem(i, nbuf)
        rows = pl.ds(pl.multiple_of(i * gb.shape[1], gb.shape[1]), gb.shape[1])
        return [pltpu.make_async_copy(r.at[at(i)], ib.at[b, n], i_sem.at[b, n]) for n, r in enumerate((w, m, v))] + [
            pltpu.make_async_copy(g.at[rows], gb.at[b], i_sem.at[b, 3])]

    def stores(i):
        b = lax.rem(i, nbuf)
        return [pltpu.make_async_copy(ob.at[b, n], r.at[at(i)], o_sem.at[b, n]) for n, r in enumerate((wo, mo, vo))]

    for i in range(nbuf):
        for t in loads(i):
            t.start()
    c = c_ref[0:1, 0:1]

    def block(i, _):
        b = lax.rem(i, nbuf)
        for t in loads(i):
            t.wait()

        @pl.when(i >= nbuf)
        def _():
            for t in stores(i - nbuf):
                t.wait()

        def update(grows, gcols, rows, cols):
            w_t = ib[b, 0, rows, cols]
            m2, v2, u = moments(w_t, gb[b, grows, gcols].astype(F32), ib[b, 1, rows, cols], ib[b, 2, rows, cols])
            ob[b, 0, rows, cols] = w_t - c * u
            ob[b, 1, rows, cols] = m2
            ob[b, 2, rows, cols] = v2

        def part(n, _):
            for q in range(4):
                lanes = pl.ds(q * 256, 256)
                if kind == 'cols':
                    off = pl.multiple_of(n * 64, 64)
                    update(pl.ds(off, 64), lanes, pl.ds(q * 256 + off, 64), slice(None))
                else:
                    rows = pl.ds(pl.multiple_of(n * 64, 64), 64)
                    update(rows, lanes, rows, lanes)
            return 0

        lax.fori_loop(0, gb.shape[1] // 64, part, 0)
        for t in stores(i):
            t.start()

        @pl.when(i + nbuf < nb)
        def _():
            for t in loads(i + nbuf):
                t.start()

        x = x_ref[...] if kind == 'cols' else x_ref[:, at(i)[0]]
        d = jnp.dot(x, ob[b, 0].astype(BF), preferred_element_type=F32)
        if kind == 'cols':
            o_ref[:, at(i)[1]] = gelu(d).astype(BF)
        else:
            @pl.when(i == 0)
            def _():
                o_ref[...] = h_ref[...] + d if has_h else d

            @pl.when(i > 0)
            def _():
                o_ref[...] += d
        return 0

    lax.fori_loop(0, nb, block, 0)
    for i in range(nb - nbuf, nb):
        for t in stores(i):
            t.wait()


def lamb(kind, w, m, v, g, c, x, h=None, size=256, nbuf=4):
    rows, cols = w.shape
    tok = x.shape[0]
    hbm = pl.BlockSpec(memory_space=pltpu.HBM)
    vm = pl.BlockSpec(memory_space=pltpu.VMEM)
    if kind == 'cols':
        nb, blk, gblk = cols // size, (rows, size), (256, 1024)
        o_shape = jax.ShapeDtypeStruct((tok, cols), BF)
    else:
        nb, blk, gblk = rows // size, (size, cols), (size, cols)
        o_shape = jax.ShapeDtypeStruct((tok, cols), F32)
    ins = [w, m, v, g, c, x] + ([] if h is None else [h])
    f = jax.ShapeDtypeStruct((rows, cols), F32)
    return pl.pallas_call(
        functools.partial(lamb_kernel, kind, nb, int(h is not None)),
        name='lamb_' + kind,
        in_specs=[hbm] * 4 + [vm] * (len(ins) - 4),
        out_specs=[hbm] * 3 + [vm],
        out_shape=[f, f, f, o_shape],
        scratch_shapes=[pltpu.VMEM((nbuf, 3) + blk, F32), pltpu.VMEM((nbuf,) + gblk, BF), pltpu.VMEM((nbuf, 3) + blk, F32),
                        pltpu.SemaphoreType.DMA((nbuf, 4)), pltpu.SemaphoreType.DMA((nbuf, 3))],
        compiler_params=pltpu.CompilerParams(vmem_limit_bytes=52 * 2 ** 20),
        cost_estimate=pl.CostEstimate(flops=40 * 10 ** 9, bytes_accessed=rows * cols * 26, transcendentals=0),
    )(*ins)


def solution(mesh):
    p = mesh.shape['data']

    def gather(s):
        return lax.all_gather(s, 'data', axis=0, tiled=True)

    def step(wi, w1, w2, mi, vi, m1, v1, m2, v2, x0, y0, x1, y1):
        w1, w2, m1, v1, m2, v2 = (t[0] for t in (w1, w2, m1, v1, m2, v2))
        d = wi.shape[1]
        s2, s1, gi, c = reduce_grads(p, x0, y0, w2, m2, v2, w1, m1, v1, wi, mi, vi)
        g1 = gather(s1)
        g2 = gather(s2)
        wi_n, mi_n, vi_n, h = lamb('in', wi, mi, vi, gi, c[1], x1)
        w1_n, m1_n, v1_n, s = lamb('cols', w1, m1, v1, g1, c[2], h.astype(BF))
        w2_n, m2_n, v2_n, h = lamb('out', w2, m2, v2, g2, c[0], s, h)
        loss = jnp.sum((h - y1.astype(F32)) ** 2, axis=-1) / (2.0 * d)
        return (wi_n, w1_n[None], w2_n[None], mi_n, vi_n, m1_n[None], v1_n[None], m2_n[None], v2_n[None], loss, h)

    w2s = P('rep', None)
    w3s = P('rep', None, None)
    ts = P(('rep', 'data'), None)
    return jax.shard_map(step, mesh=mesh,
                         in_specs=(w2s, w3s, w3s, w2s, w2s, w3s, w3s, w3s, w3s, ts, ts, ts, ts),
                         out_specs=(w2s, w3s, w3s, w2s, w2s, w3s, w3s, w3s, w3s, P(('rep', 'data')), ts),
                         check_vma=False)
```

```python
import functools

import jax
import jax.numpy as jnp
from jax import lax
from jax.experimental import pallas as pl
from jax.experimental.pallas import tpu as pltpu
from jax.sharding import PartitionSpec as P

BETA1 = 0.9
BETA2 = 0.999
BC1 = 1.0 / (1.0 - BETA1 ** 10)
BC2 = 1.0 / (1.0 - BETA2 ** 10)
EPS = 1e-12
WD = 0.01
ETA = 0.05
R2 = 0.7071067811865476
R2PI = 0.3989422804014327
BF = jnp.bfloat16
F32 = jnp.float32


def gelu(a):
    return 0.5 * a * (1.0 + lax.erf(a * R2))


def gelu_grad(a):
    return 0.5 * (1.0 + lax.erf(a * R2)) + a * jnp.exp(-0.5 * a * a) * R2PI


MESH = pl.DeviceIdType.MESH
ROUNDS = 6


def fold8(x):
    return jnp.sum(x.reshape(x.shape[0] // 8, 8, x.shape[1]), axis=0)


def moments(w, g, m, v):
    m2 = BETA1 * m + (1.0 - BETA1) * g
    v2 = BETA2 * v + (1.0 - BETA2) * g * g
    u = BC1 * m2 / (jnp.sqrt(BC2 * v2) + EPS) + WD * w
    return m2, v2, u


def sum_kernel(p, x_ref, y_ref, w2, m2, v2, w1, m1, v1, wi, mi, vi,
               o2, o1, oi, p2, p1, cs_ref,
               s_ref, gb_ref, hb_ref, a_ref, g_ref, st, pr, pt, rb, e_s, h_t, g0_s, wa, wb, lw, gst, ns, nr,
               d_send, d_recv, r_send, r_recv, credit, pcredit, w_sem, l_sem, o_sem, n_send, n_recv, a_send, a_recv, b_send, b_recv, f_sem, c_send, c_recv):
    me = lax.axis_index('data')
    core = lax.rem(me, 2)
    chip = lax.div(me, 2)
    nc = p // 2
    partner = me + 1 - 2 * core
    right = lax.rem(me + 2, p)
    left = lax.rem(me + p - 2, p)
    dims_t = (((1,), (1,)), ((), ()))

    def owner(t, k):
        return 2 * lax.rem(chip + t, nc) + k

    def remote(src, dst, ss, rs, dev):
        return pltpu.make_async_remote_copy(src_ref=src, dst_ref=dst, send_sem=ss, recv_sem=rs,
                                            device_id={'data': dev}, device_id_type=MESH)

    def d2d(b, t):
        return remote(st.at[b, t], pr.at[b, t], d_send.at[b, t], d_recv.at[b, t], partner)

    up, lo = pl.ds(0, 128), pl.ds(128, 128)
    routes = ((2, up, 0, right), (2, lo, 1, left), (1, lo, 2, right), (3, up, 3, left), (1, up, 4, right), (3, lo, 5, left))

    def ring(b, n):
        t, half, slot, dev = routes[n]
        return remote(pt.at[b, t, half], rb.at[b, slot], r_send.at[b, n], r_recv.at[b, n], dev)

    def tile(r, j, store):
        h = r % 2
        if r // 2 == 2:
            cols = pl.ds(pl.multiple_of(j * 512 + h * 256, 256), 256)
            for q in range(4):
                d = jnp.dot(h_t[q * 256:(q + 1) * 256, :], e_s[:, cols], preferred_element_type=F32)
                store(pl.ds(q * 256, 256), d.astype(BF))
        else:
            x, y = (s_ref, gb_ref) if r < 2 else (x_ref, g0_s)
            cols = pl.ds(pl.multiple_of(j * 512 + h * 256, 256), 256)
            d = jnp.dot(x[:, cols].T, y[...], preferred_element_type=F32)
            store(pl.ds(0, 1024), d.astype(BF))

    def s1(r):
        b = r % 2
        if r >= 2:
            pl.semaphore_wait(pcredit, 1)

        def pair(i, _):
            s1_pair(r, i)
            return 0

        lax.fori_loop(0, nc, pair, 0)

    def s1_pair(r, i):
        b = r % 2
        t = lax.rem(i + 2, nc)

        def theirs(cols, d):
            st[b, t, :, cols] = d

        def ours(cols, d):
            pt[b, t, :, cols] = d.astype(F32)

        tile(r, owner(t, 1 - core), theirs)
        tile(r, owner(t, core), ours)
        d2d(b, t).start()

    def s2(r):
        b = r % 2
        if r >= 2:
            pl.semaphore_wait(credit.at[0], 1)
            pl.semaphore_wait(credit.at[1], 1)
        for t in (2, 3, 1, 0):
            s2_add(r, t)
        for t in range(nc):
            d2d(b, t).wait_send()
        if r + 2 < ROUNDS:
            pl.semaphore_signal(pcredit, inc=1, device_id={'data': partner}, device_id_type=MESH)

    def s2_add(r, t):
        b = r % 2
        d2d(b, t).wait_recv()
        pt[b, t] += pr[b, t].astype(F32)
        for n in ((), (2,), (0, 1), (3,))[t]:
            ring(b, n).start()

    def s3(r):
        b = r % 2
        ring(b, 0).wait_recv()
        pt[b, 1, up] += rb[b, 0]
        ring(b, 4).start()
        ring(b, 1).wait_recv()
        pt[b, 3, lo] += rb[b, 1]
        ring(b, 5).start()

    def shard_loads(r):
        k, h = r // 2, r % 2
        out = []
        at = pl.ds(pl.multiple_of(me * 512 + h * 256, 256), 256)
        for n, ref in enumerate(((w2, m2, v2), (wi, mi, vi), (w1, m1, v1))[k]):
            if k == 2:
                for q in range(4):
                    part = pl.ds(q * 256, 256)
                    out.append(pltpu.make_async_copy(ref.at[part, at], lw.at[n, :, part], l_sem.at[n, q]))
            else:
                out.append(pltpu.make_async_copy(ref.at[at], lw.at[n], l_sem.at[n, 0]))
        return out

    def put_out(r):
        k, h = r // 2, r % 2
        rows = pl.ds(h * 256, 256)
        dst = oi.at[block(me, h)] if k == 1 else (o2, oi, o1)[k].at[rows]
        return pltpu.make_async_copy(gst.at[k, rows], dst, o_sem.at[k, h])

    def give(k, h):
        rows = pl.ds(h * 256, 256)
        return remote(gst.at[k, rows], (p2, None, p1)[k].at[rows], c_send.at[k // 2, h], c_recv.at[k // 2, h], partner)

    def block(j, h):
        return pl.ds(pl.multiple_of(j * 512 + h * 256, 256), 256)

    def ag(n):
        h = n % 2
        if n < 4:
            src, j, dev = gst.at[1, pl.ds(h * 256, 256)], me, (right, left)[n // 2]
        else:
            j, dev = (left, right)[h], (right, left)[h]
            src = oi.at[block(j, h)]
        return remote(src, oi.at[block(j, h)], a_send.at[n], a_recv.at[n], dev)

    def ag_pair(n):
        h = n % 2
        j = (me, left, right, lax.rem(me + 4, p))[n // 2]
        src = gst.at[1, pl.ds(h * 256, 256)] if n < 2 else oi.at[block(j, h)]
        return remote(src, oi.at[block(j, h)], b_send.at[n], b_recv.at[n], partner)

    def ag_own(h):
        ag(h).start()
        ag(2 + h).start()
        ag_pair(h).start()

    def ag_near(h):
        ag(h).wait_recv()
        if h == 0:
            ag(4).start()
        ag(2 + h).wait_recv()
        if h == 1:
            ag(5).start()
        ag_pair(2 + h).start()
        ag_pair(4 + h).start()

    def ag_far(h):
        ag(4 + h).wait_recv()
        ag_pair(6 + h).start()

    def s4(r):
        b, k, h = r % 2, r // 2, r % 2
        loads = shard_loads(r)
        for c in loads:
            c.start()
        for n in (2, 3, 4, 5):
            ring(b, n).wait_recv()
        gst[k, pl.ds(h * 256, 128)] = (pt[b, 0, up] + rb[b, 4] + rb[b, 3]).astype(BF)
        gst[k, pl.ds(h * 256 + 128, 128)] = (pt[b, 0, lo] + rb[b, 5] + rb[b, 2]).astype(BF)
        for n in range(6):
            ring(b, n).wait_send()
        if r + 2 < ROUNDS:
            pl.semaphore_signal(credit.at[0], inc=1, device_id={'data': right}, device_id_type=MESH)
            pl.semaphore_signal(credit.at[1], inc=1, device_id={'data': left}, device_id_type=MESH)
        for c in loads:
            c.wait()
        put_out(r).start()
        sw = jnp.zeros((8, 1024), F32)
        su = jnp.zeros((8, 1024), F32)
        for i in range(4):
            rows = pl.ds(i * 64, 64)
            w = lw[0, rows]
            _, _, u = moments(w, gst[k, pl.ds(h * 256 + i * 64, 64)].astype(F32), lw[1, rows], lw[2, rows])
            sw += fold8(w * w)
            su += fold8(u * u)
        for n, t in enumerate((sw, su)):
            f = t[:, 0:128]
            for q in range(1, 8):
                f += t[:, q * 128:(q + 1) * 128]
            row = pl.ds((2 * k + n) * 8, 8)
            if h == 0:
                ns[row] = f
            else:
                ns[row] += f

    def load_a(i):
        return pltpu.make_async_copy(w2.at[pl.ds(i * 256, 256)], wa.at[lax.rem(i, 2)], w_sem.at[lax.rem(i, 2)])

    def load_b(i):
        return pltpu.make_async_copy(w1.at[pl.ds(i * 128, 128)], wb.at[lax.rem(i, 2)], w_sem.at[lax.rem(i, 2)])

    def make_e():
        n = s_ref.shape[1] // 256
        load_a(0).start()
        h_t[...] = hb_ref[...].T

        def body(i, _):
            @pl.when(i + 1 < n)
            def _():
                load_a(i + 1).start()
            load_a(i).wait()
            cols = pl.ds(pl.multiple_of(i * 256, 256), 256)
            d = lax.dot_general(gb_ref[...], wa[lax.rem(i, 2)].astype(BF), dims_t, preferred_element_type=F32)
            e_s[:, cols] = (d * gelu_grad(a_ref[:, cols])).astype(BF)
            return 0

        lax.fori_loop(0, n, body, 0)

    def make_g0():
        n = gb_ref.shape[1] // 128
        load_b(0).start()

        def body(i, _):
            @pl.when(i + 1 < n)
            def _():
                load_b(i + 1).start()
            load_b(i).wait()
            cols = pl.ds(pl.multiple_of(i * 128, 128), 128)
            d = lax.dot_general(e_s[...], wb[lax.rem(i, 2)].astype(BF), dims_t, preferred_element_type=F32)
            g0_s[:, cols] = (g_ref[:, cols] + d).astype(BF)
            return 0

        lax.fori_loop(0, n, body, 0)

    def f_buf(u):
        return pt.at[lax.div(u, 2), pl.ds(2 * lax.rem(u, 2), 2)]

    def f_copy(src, u, n):
        return pltpu.make_async_copy(src, pt.at[lax.div(u, 2), 2 * lax.rem(u, 2) + n], f_sem.at[u, n])

    def f_start(i):
        u = lax.rem(i, 4)
        k, o = lax.div(i, 8), lax.rem(i, 8)
        for n in range(2):
            rows = pl.ds(pl.multiple_of(o * 512 + n * 256, 256), 256)

            @pl.when(k == 0)
            def _():
                f_copy(wi.at[rows], u, n).start()

            @pl.when(k == 1)
            def _():
                part = pl.ds(pl.multiple_of(lax.rem(o, 2) * 512 + n * 256, 256), 256)
                f_copy(w1.at[part, pl.ds(pl.multiple_of(lax.div(o, 2) * 1024, 1024), 1024)], u, n).start()

            @pl.when(k == 2)
            def _():
                f_copy(w2.at[rows], u, n).start()

    def f_take(i):
        u = lax.rem(i, 4)
        for n in range(2):
            f_copy(wi.at[pl.ds(0, 256)], u, n).wait()
        return f_buf(u)[...].reshape(512, 1024).astype(BF)

    def f_loop(k, body):
        def one(n, _):
            i = 8 * k + n
            body(n, f_take(i))

            @pl.when(i + 4 < 24)
            def _():
                f_start(i + 4)
            return 0

        lax.fori_loop(0, 8, one, 0)

    def chunk(n):
        return pl.ds(pl.multiple_of(n * 512, 512), 512)

    def f_in(n, w):
        d = jnp.dot(x_ref[:, chunk(n)], w, preferred_element_type=F32)

        @pl.when(n == 0)
        def _():
            g_ref[...] = d

        @pl.when(n > 0)
        def _():
            g_ref[...] += d

    def f_mid(n, w):
        cols = pl.ds(pl.multiple_of(lax.div(n, 2) * 1024, 1024), 1024)

        @pl.when(lax.rem(n, 2) == 0)
        def _():
            a_ref[:, cols] = jnp.dot(hb_ref[:, 0:512], w, preferred_element_type=F32)

        @pl.when(lax.rem(n, 2) == 1)
        def _():
            a_ref[:, cols] += jnp.dot(hb_ref[:, 512:1024], w, preferred_element_type=F32)

            def act(q, _):
                part = pl.ds(pl.multiple_of(lax.div(n, 2) * 1024 + q * 256, 256), 256)
                s_ref[:, part] = gelu(a_ref[:, part]).astype(BF)
                return 0

            lax.fori_loop(0, 4, act, 0)

    def f_out(n, w):
        g_ref[...] += jnp.dot(s_ref[:, chunk(n)], w, preferred_element_type=F32)

    barrier = pltpu.get_barrier_semaphore()
    for o in range(1, p):
        pl.semaphore_signal(barrier, inc=1, device_id={'data': lax.rem(me + o, p)}, device_id_type=MESH)
    for i in range(4):
        f_start(jnp.int32(i))
    f_loop(0, f_in)
    hb_ref[...] = g_ref[...].astype(BF)
    f_loop(1, f_mid)
    f_loop(2, f_out)
    scale = 1.0 / (x_ref.shape[0] * p * g_ref.shape[1])
    g_ref[...] = (g_ref[...] - y_ref[...].astype(F32)) * scale
    gb_ref[...] = g_ref[...].astype(BF)
    pl.semaphore_wait(barrier, p - 1)

    s1_pair(0, jnp.int32(0))
    s1_pair(0, jnp.int32(1))
    s2_add(0, 2)
    s1_pair(0, jnp.int32(2))
    s2_add(0, 3)
    s1_pair(0, jnp.int32(3))
    s2_add(0, 1)
    s2_add(0, 0)
    for t in range(nc):
        d2d(0, t).wait_send()
    pl.semaphore_signal(pcredit, inc=1, device_id={'data': partner}, device_id_type=MESH)
    for r in range(ROUNDS):
        if r + 1 < ROUNDS:
            s1(r + 1)
        s3(r)
        if r + 1 < ROUNDS:
            s2(r + 1)
        if r == 0:
            make_e()
            make_g0()
        if r == 3:
            ag_near(0)
        if r == 4:
            ag_near(1)
            ag_far(0)
        if r == 5:
            ag_far(1)
        s4(r)
        if r // 2 == 1:
            ag_own(r % 2)
        else:
            give(r // 2, r % 2).start()

    def norm(o):
        return remote(ns, nr.at[me], n_send.at[o - 1], n_recv.at[o - 1], lax.rem(me + o, p))

    nr[me] = ns[...]
    for o in range(1, p):
        norm(o).start()
    for o in range(1, p):
        norm(o).wait()
    tot = nr[0]
    for o in range(1, p):
        tot = tot + nr[o]
    for k in range(3):
        nw = jnp.sqrt(jnp.sum(tot[16 * k:16 * k + 8], keepdims=True))
        nu = jnp.sqrt(jnp.sum(tot[16 * k + 8:16 * k + 16], keepdims=True))
        cs_ref[k] = jnp.broadcast_to(ETA * (nw / nu), (8, 128))
    for r in range(ROUNDS):
        put_out(r).wait()
    for n in range(6):
        ag(n).wait_send()
    for n in range(8):
        ag_pair(n).wait()
    for n in range(4):
        give(n // 2 * 2, n % 2).wait()


def reduce_grads(p, x, y, w2, m2, v2, w1, m1, v1, wi, mi, vi):
    vm = pl.BlockSpec(memory_space=pltpu.VMEM)
    hbm = pl.BlockSpec(memory_space=pltpu.HBM)
    dma, reg = pltpu.SemaphoreType.DMA, pltpu.SemaphoreType.REGULAR
    o = jax.ShapeDtypeStruct((512, 1024), BF)
    tok = x.shape[0]
    return pl.pallas_call(
        functools.partial(sum_kernel, p),
        name='sum_grads',
        in_specs=[vm] * 2 + [hbm] * 9,
        out_specs=[hbm] * 5 + [vm],
        out_shape=[o, o, jax.ShapeDtypeStruct((512 * p, 1024), BF), o, o, jax.ShapeDtypeStruct((3, 8, 128), F32)],
        scratch_shapes=[
            pltpu.VMEM((tok, 4096), BF), pltpu.VMEM((tok, 1024), BF), pltpu.VMEM((tok, 1024), BF),
            pltpu.VMEM((tok, 4096), F32), pltpu.VMEM((tok, 1024), F32),
            pltpu.VMEM((2, 4, 256, 1024), BF), pltpu.VMEM((2, 4, 256, 1024), BF), pltpu.VMEM((2, 4, 256, 1024), F32),
            pltpu.VMEM((2, 6, 128, 1024), F32), pltpu.VMEM((tok, 4096), BF), pltpu.VMEM((1024, tok), BF),
            pltpu.VMEM((tok, 1024), BF), pltpu.VMEM((2, 256, 1024), F32), pltpu.VMEM((2, 128, 4096), F32),
            pltpu.VMEM((3, 256, 1024), F32), pltpu.VMEM((3, 512, 1024), BF), pltpu.VMEM((48, 128), F32), pltpu.VMEM((p, 48, 128), F32),
            dma((2, 4)), dma((2, 4)), dma((2, 6)), dma((2, 6)), reg((2,)), reg, dma((2,)), dma((3, 4)), dma((3, 2)),
            dma((p - 1,)), dma((p - 1,)), dma((6,)), dma((6,)), dma((8,)), dma((8,)), dma((4, 2)), dma((2, 2)), dma((2, 2)),
        ],
        compiler_params=pltpu.CompilerParams(collective_id=0, has_side_effects=True, vmem_limit_bytes=60 * 2 ** 20),
        cost_estimate=pl.CostEstimate(flops=10 ** 11, bytes_accessed=10 ** 8, transcendentals=0),
    )(x, y, w2, m2, v2, w1, m1, v1, wi, mi, vi)


def lamb_kernel(kind, part, p, nb, size, n_g, has_h, has_y, w, m, v, *refs):
    g_refs, refs = refs[:n_g], refs[n_g:]
    c_ref, x_ref, refs = refs[0], refs[1], refs[2:]
    h_ref = refs[0] if has_h else None
    y_ref = refs[has_h] if has_y else None
    l_ref, refs = (refs[-6], refs[:-6] + refs[-5:]) if has_y else (None, refs)
    wo, mo, vo, o_ref, ib, gb, ob, i_sem, o_sem = refs[-9:]
    nbuf = ib.shape[0]
    grows = gb.shape[1]
    me = lax.axis_index('data')
    core = lax.rem(me, 2)

    def which(i):
        if part == 'all':
            return i
        h = lax.rem(i, 2)
        if part == 'near':
            return 2 * (me + lax.div(i, 2) * (1 - 2 * core)) + h
        chip = lax.rem(lax.div(me, 2) + 1 + lax.div(i, 4), p // 2)
        return 4 * chip + lax.rem(i, 4)

    def at(i):
        s = pl.ds(pl.multiple_of(which(i) * size, size), size)
        return (slice(None), s) if kind == 'cols' else (s, slice(None))

    def loads(i):
        b = lax.rem(i, nbuf)
        return [pltpu.make_async_copy(r.at[at(i)], ib.at[b, n], i_sem.at[b, n]) for n, r in enumerate((w, m, v))]

    def load_g(i, ref, j):
        b = lax.rem(i, nbuf)
        rows = pl.ds(pl.multiple_of(j * grows, grows), grows)
        return pltpu.make_async_copy(ref.at[rows], gb.at[b], i_sem.at[b, 3])

    def start(i):
        for t in loads(i):
            t.start()
        if part != 'near':
            load_g(i, g_refs[0], which(i)).start()
        else:
            for n in range(2):
                @pl.when(lax.div(i, 2) == n)
                def _():
                    load_g(i, g_refs[n], lax.rem(i, 2)).start()

    def stores(i):
        b = lax.rem(i, nbuf)
        return [pltpu.make_async_copy(ob.at[b, n], r.at[at(i)], o_sem.at[b, n]) for n, r in enumerate((wo, mo, vo))]

    for i in range(nbuf):
        start(jnp.int32(i))
    c = c_ref[0:1, 0:1]
    if kind == 'cols' and has_h:
        o_ref[...] = h_ref[...]

    def block(i, _):
        b = lax.rem(i, nbuf)
        for t in loads(i):
            t.wait()
        load_g(i, g_refs[0], 0).wait()

        @pl.when(i >= nbuf)
        def _():
            for t in stores(i - nbuf):
                t.wait()

        def update(grow, gcol, rows, cols):
            w_t = ib[b, 0, rows, cols]
            m2, v2, u = moments(w_t, gb[b, grow, gcol].astype(F32), ib[b, 1, rows, cols], ib[b, 2, rows, cols])
            ob[b, 0, rows, cols] = w_t - c * u
            ob[b, 1, rows, cols] = m2
            ob[b, 2, rows, cols] = v2

        def piece(n, _):
            for q in range(4):
                lanes = pl.ds(q * 256, 256)
                off = pl.multiple_of(n * 64, 64)
                if kind == 'cols':
                    update(pl.ds(off, 64), lanes, pl.ds(q * 256 + off, 64), slice(None))
                else:
                    update(pl.ds(off, 64), lanes, pl.ds(off, 64), lanes)
            return 0

        lax.fori_loop(0, grows // 64, piece, 0)
        for t in stores(i):
            t.start()

        @pl.when(i + nbuf < nb)
        def _():
            start(i + nbuf)

        x = x_ref[...] if kind == 'cols' else x_ref[:, at(i)[0]]
        d = jnp.dot(x, ob[b, 0].astype(BF), preferred_element_type=F32)
        if kind == 'cols':
            o_ref[:, at(i)[1]] = gelu(d).astype(BF)
        else:
            @pl.when(i == 0)
            def _():
                o_ref[...] = h_ref[...] + d if has_h else d

            @pl.when(i > 0)
            def _():
                o_ref[...] += d
        return 0

    lax.fori_loop(0, nb, block, 0)
    if has_y:
        e = o_ref[...] - y_ref[...].astype(F32)
        row = jnp.sum(e * e, axis=-1, keepdims=True) / (2.0 * e.shape[1])
        l_ref[...] = jnp.broadcast_to(row, (e.shape[0], 128)).T[0:8]
    for i in range(nb - nbuf, nb):
        for t in stores(i):
            t.wait()


def lamb(kind, part, p, w, m, v, g, c, x, h=None, y=None, prev=None, size=256, nbuf=4):
    rows, cols = w.shape
    tok = x.shape[0]
    hbm = pl.BlockSpec(memory_space=pltpu.HBM)
    vm = pl.BlockSpec(memory_space=pltpu.VMEM)
    if kind == 'cols':
        nb, blk, gblk = cols // size, (rows, size), (256, 1024)
        o_shape = jax.ShapeDtypeStruct((tok, cols), BF)
    else:
        nb, blk, gblk = rows // size, (size, cols), (size, cols)
        o_shape = jax.ShapeDtypeStruct((tok, cols), F32)
    nb = {'all': nb, 'near': nb // (p // 2), 'far': nb - nb // (p // 2)}[part]
    ins = [w, m, v, *g, c, x] + [t for t in (h, y) if t is not None]
    specs = [hbm] * (3 + len(g)) + [vm] * (len(ins) - 3 - len(g))
    alias = {}
    for k, t in enumerate(prev or ()):
        alias[len(ins)] = k
        ins.append(t)
        specs.append(hbm)
    f = jax.ShapeDtypeStruct((rows, cols), F32)
    loss = [] if y is None else [jax.ShapeDtypeStruct((8, tok), F32)]
    return pl.pallas_call(
        functools.partial(lamb_kernel, kind, part, p, nb, size, len(g), int(h is not None), int(y is not None)),
        name=f'lamb_{kind}_{part}',
        in_specs=specs,
        out_specs=[hbm] * 3 + [vm] * (1 + len(loss)),
        out_shape=[f, f, f, o_shape] + loss,
        scratch_shapes=[pltpu.VMEM((nbuf, 3) + blk, F32), pltpu.VMEM((nbuf,) + gblk, BF), pltpu.VMEM((nbuf, 3) + blk, F32),
                        pltpu.SemaphoreType.DMA((nbuf, 4)), pltpu.SemaphoreType.DMA((nbuf, 3))],
        input_output_aliases=alias,
        compiler_params=pltpu.CompilerParams(vmem_limit_bytes=52 * 2 ** 20),
        cost_estimate=pl.CostEstimate(flops=25 * 10 ** 8 * nb, bytes_accessed=nb * 26 * size * 1024, transcendentals=0),
    )(*ins)


def solution(mesh):
    p = mesh.shape['data']

    def gather(s):
        return lax.all_gather(s, 'data', axis=0, tiled=True)

    def step(wi, w1, w2, mi, vi, m1, v1, m2, v2, x0, y0, x1, y1):
        w1, w2, m1, v1, m2, v2 = (t[0] for t in (w1, w2, m1, v1, m2, v2))
        s2, s1, gi, n2, n1, c = reduce_grads(p, x0, y0, w2, m2, v2, w1, m1, v1, wi, mi, vi)
        g1 = gather(s1)
        g2 = gather(s2)
        wi_n, mi_n, vi_n, h = lamb('in', 'all', p, wi, mi, vi, [gi], c[1], x1, size=128, nbuf=8)
        hb = h.astype(BF)
        *u, s = lamb('cols', 'near', p, w1, m1, v1, [s1, n1], c[2], hb)
        w1_n, m1_n, v1_n, s = lamb('cols', 'far', p, w1, m1, v1, [g1], c[2], hb, h=s, prev=u)
        *u, h = lamb('out', 'near', p, w2, m2, v2, [s2, n2], c[0], s, h=h)
        w2_n, m2_n, v2_n, h, loss = lamb('out', 'far', p, w2, m2, v2, [g2], c[0], s, h=h, y=y1, prev=u)
        loss = loss[0]
        return (wi_n, w1_n[None], w2_n[None], mi_n, vi_n, m1_n[None], v1_n[None], m2_n[None], v2_n[None], loss, h)

    w2s = P('rep', None)
    w3s = P('rep', None, None)
    ts = P(('rep', 'data'), None)
    return jax.shard_map(step, mesh=mesh,
                         in_specs=(w2s, w3s, w3s, w2s, w2s, w3s, w3s, w3s, w3s, ts, ts, ts, ts),
                         out_specs=(w2s, w3s, w3s, w2s, w2s, w3s, w3s, w3s, w3s, P(('rep', 'data')), ts),
                         check_vma=False)
```

```python
import functools

import jax
import jax.numpy as jnp
from jax import lax
from jax.experimental import pallas as pl
from jax.experimental.pallas import tpu as pltpu
from jax.sharding import PartitionSpec as P

BETA1 = 0.9
BETA2 = 0.999
BC1 = 1.0 / (1.0 - BETA1 ** 10)
BC2 = 1.0 / (1.0 - BETA2 ** 10)
EPS = 1e-12
WD = 0.01
ETA = 0.05
R2 = 0.7071067811865476
R2PI = 0.3989422804014327
BF = jnp.bfloat16
F32 = jnp.float32


def gelu(a):
    return 0.5 * a * (1.0 + lax.erf(a * R2))


def gelu_grad(a):
    return 0.5 * (1.0 + lax.erf(a * R2)) + a * jnp.exp(-0.5 * a * a) * R2PI


MESH = pl.DeviceIdType.MESH
ROUNDS = 6


def fold8(x):
    return jnp.sum(x.reshape(x.shape[0] // 8, 8, x.shape[1]), axis=0)


def moments(w, g, m, v):
    m2 = BETA1 * m + (1.0 - BETA1) * g
    v2 = BETA2 * v + (1.0 - BETA2) * g * g
    u = BC1 * m2 / (jnp.sqrt(BC2 * v2) + EPS) + WD * w
    return m2, v2, u


def sum_kernel(p, x_ref, y_ref, w2, m2, v2, w1, m1, v1, wi, mi, vi,
               o2, o1, oi, p2, p1, cs_ref,
               s_ref, gb_ref, hb_ref, a_ref, g_ref, st, pr, pt, rb, e_s, h_t, g0_s, wa, wb, lw, gst, ns, nr,
               d_send, d_recv, r_send, r_recv, credit, pcredit, w_sem, l_sem, o_sem, n_send, n_recv, a_send, a_recv, b_send, b_recv, f_sem, c_send, c_recv):
    me = lax.axis_index('data')
    core = lax.rem(me, 2)
    chip = lax.div(me, 2)
    nc = p // 2
    partner = me + 1 - 2 * core
    right = lax.rem(me + 2, p)
    left = lax.rem(me + p - 2, p)
    dims_t = (((1,), (1,)), ((), ()))

    def owner(t, k):
        return 2 * lax.rem(chip + t, nc) + k

    def remote(src, dst, ss, rs, dev):
        return pltpu.make_async_remote_copy(src_ref=src, dst_ref=dst, send_sem=ss, recv_sem=rs,
                                            device_id={'data': dev}, device_id_type=MESH)

    def d2d(b, t):
        return remote(st.at[b, t], pr.at[b, t], d_send.at[b, t], d_recv.at[b, t], partner)

    up, lo = pl.ds(0, 128), pl.ds(128, 128)
    routes = ((2, up, 0, right), (2, lo, 1, left), (1, lo, 2, right), (3, up, 3, left), (1, up, 4, right), (3, lo, 5, left))

    def ring(b, n):
        t, half, slot, dev = routes[n]
        return remote(pt.at[b, t, half], rb.at[b, slot], r_send.at[b, n], r_recv.at[b, n], dev)

    def tile(r, j, store):
        h = r % 2
        if r // 2 == 2:
            cols = pl.ds(pl.multiple_of(j * 512 + h * 256, 256), 256)
            for q in range(4):
                d = jnp.dot(h_t[q * 256:(q + 1) * 256, :], e_s[:, cols], preferred_element_type=F32)
                store(pl.ds(q * 256, 256), d.astype(BF))
        else:
            x, y = (s_ref, gb_ref) if r < 2 else (x_ref, g0_s)
            cols = pl.ds(pl.multiple_of(j * 512 + h * 256, 256), 256)
            d = jnp.dot(x[:, cols].T, y[...], preferred_element_type=F32)
            store(pl.ds(0, 1024), d.astype(BF))

    def s1(r):
        b = r % 2
        if r >= 2:
            pl.semaphore_wait(pcredit, 1)

        def pair(i, _):
            s1_pair(r, i)
            return 0

        lax.fori_loop(0, nc, pair, 0)

    def s1_pair(r, i):
        b = r % 2
        t = lax.rem(i + 2, nc)

        def theirs(cols, d):
            st[b, t, :, cols] = d

        def ours(cols, d):
            pt[b, t, :, cols] = d.astype(F32)

        tile(r, owner(t, 1 - core), theirs)
        tile(r, owner(t, core), ours)
        d2d(b, t).start()

    def s2(r):
        b = r % 2
        if r >= 2:
            pl.semaphore_wait(credit.at[0], 1)
            pl.semaphore_wait(credit.at[1], 1)
        for t in (2, 3, 1, 0):
            s2_add(r, t)
        for t in range(nc):
            d2d(b, t).wait_send()
        if r + 2 < ROUNDS:
            pl.semaphore_signal(pcredit, inc=1, device_id={'data': partner}, device_id_type=MESH)

    def s2_add(r, t):
        b = r % 2
        d2d(b, t).wait_recv()
        pt[b, t] += pr[b, t].astype(F32)
        for n in ((), (2,), (0, 1), (3,))[t]:
            ring(b, n).start()

    def s3(r):
        b = r % 2
        ring(b, 0).wait_recv()
        pt[b, 1, up] += rb[b, 0]
        ring(b, 4).start()
        ring(b, 1).wait_recv()
        pt[b, 3, lo] += rb[b, 1]
        ring(b, 5).start()

    def shard_loads(r):
        k, h = r // 2, r % 2
        out = []
        at = pl.ds(pl.multiple_of(me * 512 + h * 256, 256), 256)
        for n, ref in enumerate(((w2, m2, v2), (wi, mi, vi), (w1, m1, v1))[k]):
            if k == 2:
                for q in range(4):
                    part = pl.ds(q * 256, 256)
                    out.append(pltpu.make_async_copy(ref.at[part, at], lw.at[n, :, part], l_sem.at[n, q]))
            else:
                out.append(pltpu.make_async_copy(ref.at[at], lw.at[n], l_sem.at[n, 0]))
        return out

    def put_out(r):
        k, h = r // 2, r % 2
        rows = pl.ds(h * 256, 256)
        dst = oi.at[block(me, h)] if k == 1 else (o2, oi, o1)[k].at[rows]
        return pltpu.make_async_copy(gst.at[k, rows], dst, o_sem.at[k, h])

    def give(k, h):
        rows = pl.ds(h * 256, 256)
        return remote(gst.at[k, rows], (p2, None, p1)[k].at[rows], c_send.at[k // 2, h], c_recv.at[k // 2, h], partner)

    def block(j, h):
        return pl.ds(pl.multiple_of(j * 512 + h * 256, 256), 256)

    def ag(n):
        h = n % 2
        if n < 4:
            src, j, dev = gst.at[1, pl.ds(h * 256, 256)], me, (right, left)[n // 2]
        else:
            j, dev = (left, right)[h], (right, left)[h]
            src = oi.at[block(j, h)]
        return remote(src, oi.at[block(j, h)], a_send.at[n], a_recv.at[n], dev)

    def ag_pair(n):
        h = n % 2
        j = (me, left, right, lax.rem(me + 4, p))[n // 2]
        src = gst.at[1, pl.ds(h * 256, 256)] if n < 2 else oi.at[block(j, h)]
        return remote(src, oi.at[block(j, h)], b_send.at[n], b_recv.at[n], partner)

    def ag_own(h):
        ag(h).start()
        ag(2 + h).start()
        ag_pair(h).start()

    def ag_near(h):
        ag(h).wait_recv()
        if h == 0:
            ag(4).start()
        ag(2 + h).wait_recv()
        if h == 1:
            ag(5).start()
        ag_pair(2 + h).start()
        ag_pair(4 + h).start()

    def ag_far(h):
        ag(4 + h).wait_recv()
        ag_pair(6 + h).start()

    def s4(r):
        b, k, h = r % 2, r // 2, r % 2
        loads = shard_loads(r)
        for c in loads:
            c.start()
        for n in (2, 3, 4, 5):
            ring(b, n).wait_recv()
        gst[k, pl.ds(h * 256, 128)] = (pt[b, 0, up] + rb[b, 4] + rb[b, 3]).astype(BF)
        gst[k, pl.ds(h * 256 + 128, 128)] = (pt[b, 0, lo] + rb[b, 5] + rb[b, 2]).astype(BF)
        for n in range(6):
            ring(b, n).wait_send()
        if r + 2 < ROUNDS:
            pl.semaphore_signal(credit.at[0], inc=1, device_id={'data': right}, device_id_type=MESH)
            pl.semaphore_signal(credit.at[1], inc=1, device_id={'data': left}, device_id_type=MESH)
        for c in loads:
            c.wait()
        put_out(r).start()
        sw = jnp.zeros((8, 1024), F32)
        su = jnp.zeros((8, 1024), F32)
        for i in range(4):
            rows = pl.ds(i * 64, 64)
            w = lw[0, rows]
            _, _, u = moments(w, gst[k, pl.ds(h * 256 + i * 64, 64)].astype(F32), lw[1, rows], lw[2, rows])
            sw += fold8(w * w)
            su += fold8(u * u)
        for n, t in enumerate((sw, su)):
            f = t[:, 0:128]
            for q in range(1, 8):
                f += t[:, q * 128:(q + 1) * 128]
            row = pl.ds((2 * k + n) * 8, 8)
            if h == 0:
                ns[row] = f
            else:
                ns[row] += f

    def load_a(i):
        return pltpu.make_async_copy(w2.at[pl.ds(i * 256, 256)], wa.at[lax.rem(i, 2)], w_sem.at[lax.rem(i, 2)])

    def load_b(i):
        return pltpu.make_async_copy(w1.at[pl.ds(i * 128, 128)], wb.at[lax.rem(i, 2)], w_sem.at[lax.rem(i, 2)])

    def make_e():
        n = s_ref.shape[1] // 256
        load_a(0).start()
        h_t[...] = hb_ref[...].T

        def body(i, _):
            @pl.when(i + 1 < n)
            def _():
                load_a(i + 1).start()
            load_a(i).wait()
            cols = pl.ds(pl.multiple_of(i * 256, 256), 256)
            d = lax.dot_general(gb_ref[...], wa[lax.rem(i, 2)].astype(BF), dims_t, preferred_element_type=F32)
            e_s[:, cols] = (d * gelu_grad(a_ref[:, cols])).astype(BF)
            return 0

        lax.fori_loop(0, n, body, 0)

    def make_g0():
        n = gb_ref.shape[1] // 128
        load_b(0).start()

        def body(i, _):
            @pl.when(i + 1 < n)
            def _():
                load_b(i + 1).start()
            load_b(i).wait()
            cols = pl.ds(pl.multiple_of(i * 128, 128), 128)
            d = lax.dot_general(e_s[...], wb[lax.rem(i, 2)].astype(BF), dims_t, preferred_element_type=F32)
            g0_s[:, cols] = (g_ref[:, cols] + d).astype(BF)
            return 0

        lax.fori_loop(0, n, body, 0)

    def f_buf(u):
        return pt.at[lax.div(u, 2), pl.ds(2 * lax.rem(u, 2), 2)]

    def f_copy(src, u, n):
        return pltpu.make_async_copy(src, pt.at[lax.div(u, 2), 2 * lax.rem(u, 2) + n], f_sem.at[u, n])

    def f_start(i):
        u = lax.rem(i, 4)
        k, o = lax.div(i, 8), lax.rem(i, 8)
        for n in range(2):
            rows = pl.ds(pl.multiple_of(o * 512 + n * 256, 256), 256)

            @pl.when(k == 0)
            def _():
                f_copy(wi.at[rows], u, n).start()

            @pl.when(k == 1)
            def _():
                part = pl.ds(pl.multiple_of(lax.rem(o, 2) * 512 + n * 256, 256), 256)
                f_copy(w1.at[part, pl.ds(pl.multiple_of(lax.div(o, 2) * 1024, 1024), 1024)], u, n).start()

            @pl.when(k == 2)
            def _():
                f_copy(w2.at[rows], u, n).start()

    def f_take(i):
        u = lax.rem(i, 4)
        for n in range(2):
            f_copy(wi.at[pl.ds(0, 256)], u, n).wait()
        return f_buf(u)[...].reshape(512, 1024).astype(BF)

    def f_loop(k, body):
        def one(n, _):
            i = 8 * k + n
            body(n, f_take(i))

            @pl.when(i + 4 < 24)
            def _():
                f_start(i + 4)
            return 0

        lax.fori_loop(0, 8, one, 0)

    def chunk(n):
        return pl.ds(pl.multiple_of(n * 512, 512), 512)

    def f_in(n, w):
        d = jnp.dot(x_ref[:, chunk(n)], w, preferred_element_type=F32)

        @pl.when(n == 0)
        def _():
            g_ref[...] = d

        @pl.when(n > 0)
        def _():
            g_ref[...] += d

    def f_mid(n, w):
        cols = pl.ds(pl.multiple_of(lax.div(n, 2) * 1024, 1024), 1024)

        @pl.when(lax.rem(n, 2) == 0)
        def _():
            a_ref[:, cols] = jnp.dot(hb_ref[:, 0:512], w, preferred_element_type=F32)

        @pl.when(lax.rem(n, 2) == 1)
        def _():
            a_ref[:, cols] += jnp.dot(hb_ref[:, 512:1024], w, preferred_element_type=F32)

            def act(q, _):
                part = pl.ds(pl.multiple_of(lax.div(n, 2) * 1024 + q * 256, 256), 256)
                s_ref[:, part] = gelu(a_ref[:, part]).astype(BF)
                return 0

            lax.fori_loop(0, 4, act, 0)

    def f_out(n, w):
        g_ref[...] += jnp.dot(s_ref[:, chunk(n)], w, preferred_element_type=F32)

    barrier = pltpu.get_barrier_semaphore()
    for o in range(1, p):
        pl.semaphore_signal(barrier, inc=1, device_id={'data': lax.rem(me + o, p)}, device_id_type=MESH)
    for i in range(4):
        f_start(jnp.int32(i))
    f_loop(0, f_in)
    hb_ref[...] = g_ref[...].astype(BF)
    f_loop(1, f_mid)
    f_loop(2, f_out)
    scale = 1.0 / (x_ref.shape[0] * p * g_ref.shape[1])
    g_ref[...] = (g_ref[...] - y_ref[...].astype(F32)) * scale
    gb_ref[...] = g_ref[...].astype(BF)
    pl.semaphore_wait(barrier, p - 1)

    s1_pair(0, jnp.int32(0))
    s1_pair(0, jnp.int32(1))
    s2_add(0, 2)
    s1_pair(0, jnp.int32(2))
    s2_add(0, 3)
    s1_pair(0, jnp.int32(3))
    s2_add(0, 1)
    s2_add(0, 0)
    for t in range(nc):
        d2d(0, t).wait_send()
    pl.semaphore_signal(pcredit, inc=1, device_id={'data': partner}, device_id_type=MESH)
    for r in range(ROUNDS):
        if r + 1 < ROUNDS:
            s1(r + 1)
        s3(r)
        if r + 1 < ROUNDS:
            s2(r + 1)
        if r == 0:
            make_e()
            make_g0()
        if r == 3:
            ag_near(0)
        if r == 4:
            ag_near(1)
            ag_far(0)
        if r == 5:
            ag_far(1)
        s4(r)
        if r // 2 == 1:
            ag_own(r % 2)
        else:
            give(r // 2, r % 2).start()

    def norm(o):
        return remote(ns, nr.at[me], n_send.at[o - 1], n_recv.at[o - 1], lax.rem(me + o, p))

    nr[me] = ns[...]
    for o in range(1, p):
        norm(o).start()
    for o in range(1, p):
        norm(o).wait()
    tot = nr[0]
    for o in range(1, p):
        tot = tot + nr[o]
    for k in range(3):
        nw = jnp.sqrt(jnp.sum(tot[16 * k:16 * k + 8], keepdims=True))
        nu = jnp.sqrt(jnp.sum(tot[16 * k + 8:16 * k + 16], keepdims=True))
        cs_ref[k] = jnp.broadcast_to(ETA * (nw / nu), (8, 128))
    for r in range(ROUNDS):
        put_out(r).wait()
    for n in range(6):
        ag(n).wait_send()
    for n in range(8):
        ag_pair(n).wait()
    for n in range(4):
        give(n // 2 * 2, n % 2).wait()


def reduce_grads(p, x, y, w2, m2, v2, w1, m1, v1, wi, mi, vi):
    vm = pl.BlockSpec(memory_space=pltpu.VMEM)
    hbm = pl.BlockSpec(memory_space=pltpu.HBM)
    dma, reg = pltpu.SemaphoreType.DMA, pltpu.SemaphoreType.REGULAR
    o = jax.ShapeDtypeStruct((512, 1024), BF)
    tok = x.shape[0]
    return pl.pallas_call(
        functools.partial(sum_kernel, p),
        name='sum_grads',
        in_specs=[vm] * 2 + [hbm] * 9,
        out_specs=[hbm] * 5 + [vm],
        out_shape=[o, o, jax.ShapeDtypeStruct((512 * p, 1024), BF), o, o, jax.ShapeDtypeStruct((3, 8, 128), F32)],
        scratch_shapes=[
            pltpu.VMEM((tok, 4096), BF), pltpu.VMEM((tok, 1024), BF), pltpu.VMEM((tok, 1024), BF),
            pltpu.VMEM((tok, 4096), F32), pltpu.VMEM((tok, 1024), F32),
            pltpu.VMEM((2, 4, 256, 1024), BF), pltpu.VMEM((2, 4, 256, 1024), BF), pltpu.VMEM((2, 4, 256, 1024), F32),
            pltpu.VMEM((2, 6, 128, 1024), F32), pltpu.VMEM((tok, 4096), BF), pltpu.VMEM((1024, tok), BF),
            pltpu.VMEM((tok, 1024), BF), pltpu.VMEM((2, 256, 1024), F32), pltpu.VMEM((2, 128, 4096), F32),
            pltpu.VMEM((3, 256, 1024), F32), pltpu.VMEM((3, 512, 1024), BF), pltpu.VMEM((48, 128), F32), pltpu.VMEM((p, 48, 128), F32),
            dma((2, 4)), dma((2, 4)), dma((2, 6)), dma((2, 6)), reg((2,)), reg, dma((2,)), dma((3, 4)), dma((3, 2)),
            dma((p - 1,)), dma((p - 1,)), dma((6,)), dma((6,)), dma((8,)), dma((8,)), dma((4, 2)), dma((2, 2)), dma((2, 2)),
        ],
        compiler_params=pltpu.CompilerParams(collective_id=0, has_side_effects=True, vmem_limit_bytes=60 * 2 ** 20),
        cost_estimate=pl.CostEstimate(flops=10 ** 11, bytes_accessed=10 ** 8, transcendentals=0),
    )(x, y, w2, m2, v2, w1, m1, v1, wi, mi, vi)


def lamb_stage(kind, part, p, nb, w, m, v, g_refs, c_ref, outs, bufs, get_x, put):
    ib, gb, ob, i_sem, o_sem = bufs
    nbuf = ib.shape[0]
    me = lax.axis_index('data')
    core = lax.rem(me, 2)
    c = c_ref[0:1, 0:1]

    def which(i):
        if part == 'all':
            return i
        if part == 'near':
            return 2 * (me + lax.div(i, 2) * (1 - 2 * core)) + lax.rem(i, 2)
        chip = lax.rem(lax.div(me, 2) + 1 + lax.div(i, 4), p // 2)
        return 4 * chip + lax.rem(i, 4)

    def span(i):
        return pl.ds(pl.multiple_of(i * 256, 256), 256)

    def at(i):
        s = span(which(i))
        return (slice(None), s) if kind == 'cols' else (s, slice(None))

    def loads(i):
        b = lax.rem(i, nbuf)
        return [pltpu.make_async_copy(r.at[at(i)], ib.at[b, n], i_sem.at[b, n]) for n, r in enumerate((w, m, v))]

    def load_g(i, ref, j):
        b = lax.rem(i, nbuf)
        return pltpu.make_async_copy(ref.at[span(j)], gb.at[b], i_sem.at[b, 3])

    def start(i):
        for t in loads(i):
            t.start()
        if part != 'near':
            load_g(i, g_refs[0], which(i)).start()
        else:
            for n in range(2):
                @pl.when(lax.div(i, 2) == n)
                def _():
                    load_g(i, g_refs[n], lax.rem(i, 2)).start()

    def stores(i):
        b = lax.rem(i, nbuf)
        return [pltpu.make_async_copy(ob.at[b, n], r.at[at(i)], o_sem.at[b, n]) for n, r in enumerate(outs)]

    def run(start_next=None):
        def block(i, _):
            b = lax.rem(i, nbuf)
            for t in loads(i):
                t.wait()
            load_g(i, g_refs[0], 0).wait()

            @pl.when(i >= nbuf)
            def _():
                for t in stores(i - nbuf):
                    t.wait()

            def update(grow, gcol, rows, cols):
                w_t = ib[b, 0, rows, cols]
                m2, v2, u = moments(w_t, gb[b, grow, gcol].astype(F32), ib[b, 1, rows, cols], ib[b, 2, rows, cols])
                ob[b, 0, rows, cols] = w_t - c * u
                ob[b, 1, rows, cols] = m2
                ob[b, 2, rows, cols] = v2

            def piece(n, _):
                for q in range(4):
                    lanes = pl.ds(q * 256, 256)
                    off = pl.multiple_of(n * 64, 64)
                    if kind == 'cols':
                        update(pl.ds(off, 64), lanes, pl.ds(q * 256 + off, 64), slice(None))
                    else:
                        update(pl.ds(off, 64), lanes, pl.ds(off, 64), lanes)
                return 0

            lax.fori_loop(0, 4, piece, 0)
            for t in stores(i):
                t.start()

            @pl.when(i + nbuf < nb)
            def _():
                start(i + nbuf)

            if start_next is not None:
                @pl.when(i + nbuf >= nb)
                def _():
                    start_next(i + nbuf - nb)

            s = span(which(i))
            put(i, s, jnp.dot(get_x(s), ob[b, 0].astype(BF), preferred_element_type=F32))
            return 0

        lax.fori_loop(0, nb, block, 0)

    def drain():
        for i in range(nb - nbuf, nb):
            for t in stores(i):
                t.wait()

    return start, run, drain


def adder(o_ref, h_ref=None):
    def put(i, s, d):
        @pl.when(i == 0)
        def _():
            o_ref[...] = d if h_ref is None else h_ref[...] + d

        @pl.when(i > 0)
        def _():
            o_ref[...] += d
    return put


def setter(o_ref):
    def put(i, s, d):
        o_ref[:, s] = gelu(d).astype(BF)
    return put


def lamb_a(p, wi, mi, vi, gi, w1, m1, v1, s1, n1, ci, c1, x_ref, wio, mio, vio, w1o, m1o, v1o, h_ref, s_ref, hb, *bufs):
    nbuf = bufs[0].shape[0]
    start, run, drain = lamb_stage('in', 'all', p, wi.shape[0] // 256, wi, mi, vi, (gi,), ci, (wio, mio, vio), bufs[:5],
                                   lambda s: x_ref[:, s], adder(h_ref))
    start2, run2, drain2 = lamb_stage('cols', 'near', p, 4, w1, m1, v1, (s1, n1), c1, (w1o, m1o, v1o), bufs[5:],
                                      lambda s: hb[...], setter(s_ref))
    for i in range(nbuf):
        start(jnp.int32(i))
    run(start2)
    hb[...] = h_ref[...].astype(BF)
    run2()
    drain()
    drain2()


def lamb_b(p, w1, m1, v1, g1, w2, m2, v2, s2, n2, pw, pm, pv, c1, c2, h0_ref, s0_ref,
           w1o, m1o, v1o, w2o, m2o, v2o, s_ref, h_ref, hb, *bufs):
    nbuf = bufs[0].shape[0]
    start, run, drain = lamb_stage('cols', 'far', p, w1.shape[1] // 256 - 4, w1, m1, v1, (g1,), c1, (w1o, m1o, v1o), bufs[:5],
                                   lambda s: hb[...], setter(s_ref))
    start2, run2, drain2 = lamb_stage('out', 'near', p, 4, w2, m2, v2, (s2, n2), c2, (w2o, m2o, v2o), bufs[5:],
                                      lambda s: s_ref[:, s], adder(h_ref, h0_ref))
    for i in range(nbuf):
        start(jnp.int32(i))
    s_ref[...] = s0_ref[...]
    hb[...] = h0_ref[...].astype(BF)
    run(start2)
    run2()
    drain()
    drain2()


def lamb_c(p, w2, m2, v2, g2, pw, pm, pv, c2, s_ref, h0_ref, y_ref, w2o, m2o, v2o, h_ref, l_ref, *bufs):
    start, run, drain = lamb_stage('out', 'far', p, w2.shape[0] // 256 - 4, w2, m2, v2, (g2,), c2, (w2o, m2o, v2o), bufs,
                                   lambda s: s_ref[:, s], adder(h_ref, h0_ref))
    for i in range(bufs[0].shape[0]):
        start(jnp.int32(i))
    run()
    e = h_ref[...] - y_ref[...].astype(F32)
    row = jnp.sum(e * e, axis=-1, keepdims=True) / (2.0 * e.shape[1])
    l_ref[...] = jnp.broadcast_to(row, (e.shape[0], 128)).T[0:8]
    drain()


def lamb_call(body, name, p, n_hbm, out_hbm, out_vm, kinds, nbuf, blocks, alias, *ins):
    hbm = pl.BlockSpec(memory_space=pltpu.HBM)
    vm = pl.BlockSpec(memory_space=pltpu.VMEM)
    tok = ins[-1].shape[0]
    scratch = [pltpu.VMEM((tok, 1024), BF)] if len(kinds) > 1 else []
    for k in kinds:
        blk = (1024, 256) if k == 'cols' else (256, 1024)
        scratch += [pltpu.VMEM((nbuf, 3) + blk, F32), pltpu.VMEM((nbuf, 256, 1024), BF), pltpu.VMEM((nbuf, 3) + blk, F32),
                    pltpu.SemaphoreType.DMA((nbuf, 4)), pltpu.SemaphoreType.DMA((nbuf, 3))]
    return pl.pallas_call(
        functools.partial(body, p), name=name,
        in_specs=[hbm] * n_hbm + [vm] * (len(ins) - n_hbm),
        out_specs=[hbm] * len(out_hbm) + [vm] * len(out_vm),
        out_shape=[jax.ShapeDtypeStruct(t.shape, F32) for t in out_hbm] + list(out_vm),
        scratch_shapes=scratch,
        input_output_aliases=alias,
        compiler_params=pltpu.CompilerParams(vmem_limit_bytes=54 * 2 ** 20),
        cost_estimate=pl.CostEstimate(flops=25 * 10 ** 8 * blocks, bytes_accessed=blocks * 26 * 2 ** 18, transcendentals=0),
    )(*ins)


def solution(mesh):
    p = mesh.shape['data']

    def gather(s):
        return lax.all_gather(s, 'data', axis=0, tiled=True)

    def step(wi, w1, w2, mi, vi, m1, v1, m2, v2, x0, y0, x1, y1):
        w1, w2, m1, v1, m2, v2 = (t[0] for t in (w1, w2, m1, v1, m2, v2))
        s2, s1, gi, n2, n1, c = reduce_grads(p, x0, y0, w2, m2, v2, w1, m1, v1, wi, mi, vi)
        g1 = gather(s1)
        g2 = gather(s2)
        tok, d = y0.shape
        hs = jax.ShapeDtypeStruct((tok, d), F32)
        ss = jax.ShapeDtypeStruct((tok, w1.shape[1]), BF)
        ls = jax.ShapeDtypeStruct((8, tok), F32)
        wi_n, mi_n, vi_n, *u, h, s = lamb_call(
            lamb_a, 'lamb_a', p, 9, (wi, mi, vi, w1, m1, v1), (hs, ss), ('in', 'cols'), 3, 20, {},
            wi, mi, vi, gi, w1, m1, v1, s1, n1, c[1], c[2], x1)
        w1_n, m1_n, v1_n, *u, s, h = lamb_call(
            lamb_b, 'lamb_b', p, 12, (w1, m1, v1, w2, m2, v2), (ss, hs), ('cols', 'out'), 3, 16, {9: 0, 10: 1, 11: 2},
            w1, m1, v1, g1, w2, m2, v2, s2, n2, *u, c[2], c[0], h, s)
        w2_n, m2_n, v2_n, h, loss = lamb_call(
            lamb_c, 'lamb_c', p, 7, (w2, m2, v2), (hs, ls), ('out',), 4, 12, {4: 0, 5: 1, 6: 2},
            w2, m2, v2, g2, *u, c[0], s, h, y1)
        loss = loss[0]
        return (wi_n, w1_n[None], w2_n[None], mi_n, vi_n, m1_n[None], v1_n[None], m2_n[None], v2_n[None], loss, h)

    w2s = P('rep', None)
    w3s = P('rep', None, None)
    ts = P(('rep', 'data'), None)
    return jax.shard_map(step, mesh=mesh,
                         in_specs=(w2s, w3s, w3s, w2s, w2s, w3s, w3s, w3s, w3s, ts, ts, ts, ts),
                         out_specs=(w2s, w3s, w3s, w2s, w2s, w3s, w3s, w3s, w3s, P(('rep', 'data')), ts),
                         check_vma=False)
```

```python
import functools

import jax
import jax.numpy as jnp
from jax import lax
from jax.experimental import pallas as pl
from jax.experimental.pallas import tpu as pltpu
from jax.sharding import PartitionSpec as P

BETA1 = 0.9
BETA2 = 0.999
BC1 = 1.0 / (1.0 - BETA1 ** 10)
BC2 = 1.0 / (1.0 - BETA2 ** 10)
EPS = 1e-12
WD = 0.01
ETA = 0.05
R2 = 0.7071067811865476
R2PI = 0.3989422804014327
BF = jnp.bfloat16
F32 = jnp.float32


def gelu(a):
    return 0.5 * a * (1.0 + lax.erf(a * R2))


def gelu_grad(a):
    return 0.5 * (1.0 + lax.erf(a * R2)) + a * jnp.exp(-0.5 * a * a) * R2PI


MESH = pl.DeviceIdType.MESH
ROUNDS = 6


def fold8(x):
    return jnp.sum(x.reshape(x.shape[0] // 8, 8, x.shape[1]), axis=0)


def moments(w, g, m, v):
    m2 = BETA1 * m + (1.0 - BETA1) * g
    v2 = BETA2 * v + (1.0 - BETA2) * g * g
    u = BC1 * m2 / (jnp.sqrt(BC2 * v2) + EPS) + WD * w
    return m2, v2, u


def sum_kernel(p, x_ref, y_ref, w2, m2, v2, w1, m1, v1, wi, mi, vi,
               o2, o1, oi, p2, p1, qa, qb, cs_ref,
               s_ref, gb_ref, hb_ref, a_ref, g_ref, st, pr, pt, rb, e_s, h_t, g0_s, wa, wb, lw, gst, ns, nr,
               d_send, d_recv, r_send, r_recv, credit, pcredit, w_sem, l_sem, o_sem, n_send, n_recv, a_send, a_recv, b_send, b_recv, f_sem, c_send, c_recv, q_sem):
    me = lax.axis_index('data')
    core = lax.rem(me, 2)
    chip = lax.div(me, 2)
    nc = p // 2
    partner = me + 1 - 2 * core
    right = lax.rem(me + 2, p)
    left = lax.rem(me + p - 2, p)
    dims_t = (((1,), (1,)), ((), ()))

    def owner(t, k):
        return 2 * lax.rem(chip + t, nc) + k

    def remote(src, dst, ss, rs, dev):
        return pltpu.make_async_remote_copy(src_ref=src, dst_ref=dst, send_sem=ss, recv_sem=rs,
                                            device_id={'data': dev}, device_id_type=MESH)

    def d2d(b, t):
        return remote(st.at[b, t], pr.at[b, t], d_send.at[b, t], d_recv.at[b, t], partner)

    up, lo = pl.ds(0, 128), pl.ds(128, 128)
    routes = ((2, up, 0, right), (2, lo, 1, left), (1, lo, 2, right), (3, up, 3, left), (1, up, 4, right), (3, lo, 5, left))

    def ring(b, n):
        t, half, slot, dev = routes[n]
        return remote(pt.at[b, t, half], rb.at[b, slot], r_send.at[b, n], r_recv.at[b, n], dev)

    def tile(r, j, store):
        h = r % 2
        if r // 2 == 2:
            cols = pl.ds(pl.multiple_of(j * 512 + h * 256, 256), 256)
            for q in range(4):
                d = jnp.dot(h_t[q * 256:(q + 1) * 256, :], e_s[:, cols], preferred_element_type=F32)
                store(pl.ds(q * 256, 256), d.astype(BF))
        else:
            x, y = (s_ref, gb_ref) if r < 2 else (x_ref, g0_s)
            cols = pl.ds(pl.multiple_of(j * 512 + h * 256, 256), 256)
            d = jnp.dot(x[:, cols].T, y[...], preferred_element_type=F32)
            store(pl.ds(0, 1024), d.astype(BF))

    def s1(r):
        b = r % 2
        if r >= 2:
            pl.semaphore_wait(pcredit, 1)

        def pair(i, _):
            s1_pair(r, i)
            return 0

        lax.fori_loop(0, nc, pair, 0)

    def s1_pair(r, i):
        b = r % 2
        t = lax.rem(i + 2, nc)

        def theirs(cols, d):
            st[b, t, :, cols] = d

        def ours(cols, d):
            pt[b, t, :, cols] = d.astype(F32)

        tile(r, owner(t, 1 - core), theirs)
        tile(r, owner(t, core), ours)
        d2d(b, t).start()

    def s2(r):
        b = r % 2
        if r >= 2:
            pl.semaphore_wait(credit.at[0], 1)
            pl.semaphore_wait(credit.at[1], 1)
        for t in (2, 3, 1, 0):
            s2_add(r, t)
        for t in range(nc):
            d2d(b, t).wait_send()
        if r + 2 < ROUNDS:
            pl.semaphore_signal(pcredit, inc=1, device_id={'data': partner}, device_id_type=MESH)

    def s2_add(r, t):
        b = r % 2
        d2d(b, t).wait_recv()
        pt[b, t] += pr[b, t].astype(F32)
        for n in ((), (2,), (0, 1), (3,))[t]:
            ring(b, n).start()

    def s3(r):
        b = r % 2
        ring(b, 0).wait_recv()
        pt[b, 1, up] += rb[b, 0]
        ring(b, 4).start()
        ring(b, 1).wait_recv()
        pt[b, 3, lo] += rb[b, 1]
        ring(b, 5).start()

    def shard_loads(r):
        k, h = r // 2, r % 2
        out = []
        at = pl.ds(pl.multiple_of(me * 512 + h * 256, 256), 256)
        for n, ref in enumerate(((w2, m2, v2), (wi, mi, vi), (w1, m1, v1))[k]):
            if k == 2:
                for q in range(4):
                    part = pl.ds(q * 256, 256)
                    out.append(pltpu.make_async_copy(ref.at[part, at], lw.at[n, :, part], l_sem.at[n, q]))
            else:
                out.append(pltpu.make_async_copy(ref.at[at], lw.at[n], l_sem.at[n, 0]))
        return out

    def put_out(r):
        k, h = r // 2, r % 2
        rows = pl.ds(h * 256, 256)
        dst = oi.at[block(me, h)] if k == 1 else (o2, oi, o1)[k].at[rows]
        return pltpu.make_async_copy(gst.at[k, rows], dst, o_sem.at[k, h])

    def half_out(h):
        return pltpu.make_async_copy(gst.at[0, pl.ds(h * 256, 256)], (qa, qb)[h], q_sem.at[h])

    def give(k, h):
        rows = pl.ds(h * 256, 256)
        return remote(gst.at[k, rows], (p2, None, p1)[k].at[rows], c_send.at[k // 2, h], c_recv.at[k // 2, h], partner)

    def block(j, h):
        return pl.ds(pl.multiple_of(j * 512 + h * 256, 256), 256)

    def ag(n):
        h = n % 2
        if n < 4:
            src, j, dev = gst.at[1, pl.ds(h * 256, 256)], me, (right, left)[n // 2]
        else:
            j, dev = (left, right)[h], (right, left)[h]
            src = oi.at[block(j, h)]
        return remote(src, oi.at[block(j, h)], a_send.at[n], a_recv.at[n], dev)

    def ag_pair(n):
        h = n % 2
        j = (me, left, right, lax.rem(me + 4, p))[n // 2]
        src = gst.at[1, pl.ds(h * 256, 256)] if n < 2 else oi.at[block(j, h)]
        return remote(src, oi.at[block(j, h)], b_send.at[n], b_recv.at[n], partner)

    def ag_own(h):
        ag(h).start()
        ag(2 + h).start()
        ag_pair(h).start()

    def ag_near(h):
        ag(h).wait_recv()
        if h == 0:
            ag(4).start()
        ag(2 + h).wait_recv()
        if h == 1:
            ag(5).start()
        ag_pair(2 + h).start()
        ag_pair(4 + h).start()

    def ag_far(h):
        ag(4 + h).wait_recv()
        ag_pair(6 + h).start()

    def s4(r):
        b, k, h = r % 2, r // 2, r % 2
        loads = shard_loads(r)
        for c in loads:
            c.start()
        for n in (2, 3, 4, 5):
            ring(b, n).wait_recv()
        gst[k, pl.ds(h * 256, 128)] = (pt[b, 0, up] + rb[b, 4] + rb[b, 3]).astype(BF)
        gst[k, pl.ds(h * 256 + 128, 128)] = (pt[b, 0, lo] + rb[b, 5] + rb[b, 2]).astype(BF)
        for n in range(6):
            ring(b, n).wait_send()
        if r + 2 < ROUNDS:
            pl.semaphore_signal(credit.at[0], inc=1, device_id={'data': right}, device_id_type=MESH)
            pl.semaphore_signal(credit.at[1], inc=1, device_id={'data': left}, device_id_type=MESH)
        for c in loads:
            c.wait()
        put_out(r).start()
        sw = jnp.zeros((8, 1024), F32)
        su = jnp.zeros((8, 1024), F32)
        for i in range(4):
            rows = pl.ds(i * 64, 64)
            w = lw[0, rows]
            _, _, u = moments(w, gst[k, pl.ds(h * 256 + i * 64, 64)].astype(F32), lw[1, rows], lw[2, rows])
            sw += fold8(w * w)
            su += fold8(u * u)
        for n, t in enumerate((sw, su)):
            f = t[:, 0:128]
            for q in range(1, 8):
                f += t[:, q * 128:(q + 1) * 128]
            row = pl.ds((2 * k + n) * 8, 8)
            if h == 0:
                ns[row] = f
            else:
                ns[row] += f

    def load_a(i):
        return pltpu.make_async_copy(w2.at[pl.ds(i * 256, 256)], wa.at[lax.rem(i, 2)], w_sem.at[lax.rem(i, 2)])

    def load_b(i):
        return pltpu.make_async_copy(w1.at[pl.ds(i * 128, 128)], wb.at[lax.rem(i, 2)], w_sem.at[lax.rem(i, 2)])

    def make_e():
        n = s_ref.shape[1] // 256
        load_a(0).start()
        h_t[...] = hb_ref[...].T

        def body(i, _):
            @pl.when(i + 1 < n)
            def _():
                load_a(i + 1).start()
            load_a(i).wait()
            cols = pl.ds(pl.multiple_of(i * 256, 256), 256)
            d = lax.dot_general(gb_ref[...], wa[lax.rem(i, 2)].astype(BF), dims_t, preferred_element_type=F32)
            e_s[:, cols] = (d * gelu_grad(a_ref[:, cols])).astype(BF)
            return 0

        lax.fori_loop(0, n, body, 0)

    def make_g0():
        n = gb_ref.shape[1] // 128
        load_b(0).start()

        def body(i, _):
            @pl.when(i + 1 < n)
            def _():
                load_b(i + 1).start()
            load_b(i).wait()
            cols = pl.ds(pl.multiple_of(i * 128, 128), 128)
            d = lax.dot_general(e_s[...], wb[lax.rem(i, 2)].astype(BF), dims_t, preferred_element_type=F32)
            g0_s[:, cols] = (g_ref[:, cols] + d).astype(BF)
            return 0

        lax.fori_loop(0, n, body, 0)

    def f_buf(u):
        return pt.at[lax.div(u, 2), pl.ds(2 * lax.rem(u, 2), 2)]

    def f_copy(src, u, n):
        return pltpu.make_async_copy(src, pt.at[lax.div(u, 2), 2 * lax.rem(u, 2) + n], f_sem.at[u, n])

    def f_start(i):
        u = lax.rem(i, 4)
        k, o = lax.div(i, 8), lax.rem(i, 8)
        for n in range(2):
            rows = pl.ds(pl.multiple_of(o * 512 + n * 256, 256), 256)

            @pl.when(k == 0)
            def _():
                f_copy(wi.at[rows], u, n).start()

            @pl.when(k == 1)
            def _():
                part = pl.ds(pl.multiple_of(lax.rem(o, 2) * 512 + n * 256, 256), 256)
                f_copy(w1.at[part, pl.ds(pl.multiple_of(lax.div(o, 2) * 1024, 1024), 1024)], u, n).start()

            @pl.when(k == 2)
            def _():
                f_copy(w2.at[rows], u, n).start()

    def f_take(i):
        u = lax.rem(i, 4)
        for n in range(2):
            f_copy(wi.at[pl.ds(0, 256)], u, n).wait()
        return f_buf(u)[...].reshape(512, 1024).astype(BF)

    def f_loop(k, body):
        def one(n, _):
            i = 8 * k + n
            body(n, f_take(i))

            @pl.when(i + 4 < 24)
            def _():
                f_start(i + 4)
            return 0

        lax.fori_loop(0, 8, one, 0)

    def chunk(n):
        return pl.ds(pl.multiple_of(n * 512, 512), 512)

    def f_in(n, w):
        d = jnp.dot(x_ref[:, chunk(n)], w, preferred_element_type=F32)

        @pl.when(n == 0)
        def _():
            g_ref[...] = d

        @pl.when(n > 0)
        def _():
            g_ref[...] += d

    def f_mid(n, w):
        cols = pl.ds(pl.multiple_of(lax.div(n, 2) * 1024, 1024), 1024)

        @pl.when(lax.rem(n, 2) == 0)
        def _():
            a_ref[:, cols] = jnp.dot(hb_ref[:, 0:512], w, preferred_element_type=F32)

        @pl.when(lax.rem(n, 2) == 1)
        def _():
            a_ref[:, cols] += jnp.dot(hb_ref[:, 512:1024], w, preferred_element_type=F32)

            def act(q, _):
                part = pl.ds(pl.multiple_of(lax.div(n, 2) * 1024 + q * 256, 256), 256)
                s_ref[:, part] = gelu(a_ref[:, part]).astype(BF)
                return 0

            lax.fori_loop(0, 4, act, 0)

    def f_out(n, w):
        g_ref[...] += jnp.dot(s_ref[:, chunk(n)], w, preferred_element_type=F32)

    barrier = pltpu.get_barrier_semaphore()
    for o in range(1, p):
        pl.semaphore_signal(barrier, inc=1, device_id={'data': lax.rem(me + o, p)}, device_id_type=MESH)
    for i in range(4):
        f_start(jnp.int32(i))
    f_loop(0, f_in)
    hb_ref[...] = g_ref[...].astype(BF)
    f_loop(1, f_mid)
    f_loop(2, f_out)
    scale = 1.0 / (x_ref.shape[0] * p * g_ref.shape[1])
    g_ref[...] = (g_ref[...] - y_ref[...].astype(F32)) * scale
    gb_ref[...] = g_ref[...].astype(BF)
    pl.semaphore_wait(barrier, p - 1)

    s1_pair(0, jnp.int32(0))
    s1_pair(0, jnp.int32(1))
    s2_add(0, 2)
    s1_pair(0, jnp.int32(2))
    s2_add(0, 3)
    s1_pair(0, jnp.int32(3))
    s2_add(0, 1)
    s2_add(0, 0)
    for t in range(nc):
        d2d(0, t).wait_send()
    pl.semaphore_signal(pcredit, inc=1, device_id={'data': partner}, device_id_type=MESH)
    for r in range(ROUNDS):
        if r + 1 < ROUNDS:
            s1(r + 1)
        s3(r)
        if r + 1 < ROUNDS:
            s2(r + 1)
        if r == 0:
            make_e()
            make_g0()
        if r == 3:
            ag_near(0)
        if r == 4:
            ag_near(1)
            ag_far(0)
        if r == 5:
            ag_far(1)
        s4(r)
        if r // 2 == 1:
            ag_own(r % 2)
        else:
            give(r // 2, r % 2).start()
        if r < 2:
            half_out(r).start()

    def norm(o):
        return remote(ns, nr.at[me], n_send.at[o - 1], n_recv.at[o - 1], lax.rem(me + o, p))

    nr[me] = ns[...]
    for o in range(1, p):
        norm(o).start()
    for o in range(1, p):
        norm(o).wait()
    tot = nr[0]
    for o in range(1, p):
        tot = tot + nr[o]
    for k in range(3):
        nw = jnp.sqrt(jnp.sum(tot[16 * k:16 * k + 8], keepdims=True))
        nu = jnp.sqrt(jnp.sum(tot[16 * k + 8:16 * k + 16], keepdims=True))
        cs_ref[k] = jnp.broadcast_to(ETA * (nw / nu), (8, 128))
    for r in range(ROUNDS):
        put_out(r).wait()
    for n in range(6):
        ag(n).wait_send()
    for n in range(8):
        ag_pair(n).wait()
    for n in range(4):
        give(n // 2 * 2, n % 2).wait()
    for h in range(2):
        half_out(h).wait()


def reduce_grads(p, x, y, w2, m2, v2, w1, m1, v1, wi, mi, vi):
    vm = pl.BlockSpec(memory_space=pltpu.VMEM)
    hbm = pl.BlockSpec(memory_space=pltpu.HBM)
    dma, reg = pltpu.SemaphoreType.DMA, pltpu.SemaphoreType.REGULAR
    o = jax.ShapeDtypeStruct((512, 1024), BF)
    tok = x.shape[0]
    return pl.pallas_call(
        functools.partial(sum_kernel, p),
        name='sum_grads',
        in_specs=[vm] * 2 + [hbm] * 9,
        out_specs=[hbm] * 7 + [vm],
        out_shape=[o, o, jax.ShapeDtypeStruct((512 * p, 1024), BF), o, o] + [jax.ShapeDtypeStruct((256, 1024), BF)] * 2 + [jax.ShapeDtypeStruct((3, 8, 128), F32)],
        scratch_shapes=[
            pltpu.VMEM((tok, 4096), BF), pltpu.VMEM((tok, 1024), BF), pltpu.VMEM((tok, 1024), BF),
            pltpu.VMEM((tok, 4096), F32), pltpu.VMEM((tok, 1024), F32),
            pltpu.VMEM((2, 4, 256, 1024), BF), pltpu.VMEM((2, 4, 256, 1024), BF), pltpu.VMEM((2, 4, 256, 1024), F32),
            pltpu.VMEM((2, 6, 128, 1024), F32), pltpu.VMEM((tok, 4096), BF), pltpu.VMEM((1024, tok), BF),
            pltpu.VMEM((tok, 1024), BF), pltpu.VMEM((2, 256, 1024), F32), pltpu.VMEM((2, 128, 4096), F32),
            pltpu.VMEM((3, 256, 1024), F32), pltpu.VMEM((3, 512, 1024), BF), pltpu.VMEM((48, 128), F32), pltpu.VMEM((p, 48, 128), F32),
            dma((2, 4)), dma((2, 4)), dma((2, 6)), dma((2, 6)), reg((2,)), reg, dma((2,)), dma((3, 4)), dma((3, 2)),
            dma((p - 1,)), dma((p - 1,)), dma((6,)), dma((6,)), dma((8,)), dma((8,)), dma((4, 2)), dma((2, 2)), dma((2, 2)), dma((2,)),
        ],
        compiler_params=pltpu.CompilerParams(collective_id=0, has_side_effects=True, vmem_limit_bytes=60 * 2 ** 20),
        cost_estimate=pl.CostEstimate(flops=10 ** 11, bytes_accessed=10 ** 8, transcendentals=0),
    )(x, y, w2, m2, v2, w1, m1, v1, wi, mi, vi)


def lamb_stage(kind, part, p, nb, w, m, v, g_refs, c_ref, outs, bufs, get_x, put):
    ib, gb, ob, i_sem, o_sem = bufs
    nbuf = ib.shape[0]
    me = lax.axis_index('data')
    core = lax.rem(me, 2)
    c = c_ref[0:1, 0:1]

    def which(i):
        if part == 'all':
            return i
        if part == 'near':
            return 2 * (me + lax.div(i, 2) * (1 - 2 * core)) + lax.rem(i, 2)
        if part == 'far':
            chip = lax.rem(lax.div(me, 2) + 1 + lax.div(i, 4), p // 2)
            return 4 * chip + lax.rem(i, 4)
        return 2 * shard(i) + (part == 'far1')

    def shard(i):
        return 2 * lax.rem(lax.div(me, 2) + 1 + lax.div(i, 2), p // 2) + lax.rem(i, 2)

    def span(i):
        return pl.ds(pl.multiple_of(i * 256, 256), 256)

    def at(i):
        s = span(which(i))
        return (slice(None), s) if kind == 'cols' else (s, slice(None))

    def loads(i):
        b = lax.rem(i, nbuf)
        return [pltpu.make_async_copy(r.at[at(i)], ib.at[b, n], i_sem.at[b, n]) for n, r in enumerate((w, m, v))]

    def load_g(i, ref, j):
        b = lax.rem(i, nbuf)
        return pltpu.make_async_copy(ref.at[span(j)], gb.at[b], i_sem.at[b, 3])

    def start(i):
        for t in loads(i):
            t.start()
        if part != 'near':
            load_g(i, g_refs[0], shard(i) if part in ('far0', 'far1') else which(i)).start()
        else:
            for n in range(2):
                @pl.when(lax.div(i, 2) == n)
                def _():
                    load_g(i, g_refs[n], lax.rem(i, 2)).start()

    def stores(i):
        b = lax.rem(i, nbuf)
        return [pltpu.make_async_copy(ob.at[b, n], r.at[at(i)], o_sem.at[b, n]) for n, r in enumerate(outs)]

    def run(start_next=None):
        def block(i, _):
            b = lax.rem(i, nbuf)
            for t in loads(i):
                t.wait()
            load_g(i, g_refs[0], 0).wait()

            @pl.when(i >= nbuf)
            def _():
                for t in stores(i - nbuf):
                    t.wait()

            def update(grow, gcol, rows, cols):
                w_t = ib[b, 0, rows, cols]
                m2, v2, u = moments(w_t, gb[b, grow, gcol].astype(F32), ib[b, 1, rows, cols], ib[b, 2, rows, cols])
                ob[b, 0, rows, cols] = w_t - c * u
                ob[b, 1, rows, cols] = m2
                ob[b, 2, rows, cols] = v2

            def piece(n, _):
                for q in range(4):
                    lanes = pl.ds(q * 256, 256)
                    off = pl.multiple_of(n * 64, 64)
                    if kind == 'cols':
                        update(pl.ds(off, 64), lanes, pl.ds(q * 256 + off, 64), slice(None))
                    else:
                        update(pl.ds(off, 64), lanes, pl.ds(off, 64), lanes)
                return 0

            lax.fori_loop(0, 4, piece, 0)
            for t in stores(i):
                t.start()

            @pl.when(i + nbuf < nb)
            def _():
                start(i + nbuf)

            if start_next is not None:
                @pl.when(i + nbuf >= nb)
                def _():
                    start_next(i + nbuf - nb)

            s = span(which(i))
            put(i, s, jnp.dot(get_x(s), ob[b, 0].astype(BF), preferred_element_type=F32))
            return 0

        lax.fori_loop(0, nb, block, 0)

    def drain():
        for i in range(nb - nbuf, nb):
            for t in stores(i):
                t.wait()

    return start, run, drain


def adder(o_ref, h_ref=None):
    def put(i, s, d):
        @pl.when(i == 0)
        def _():
            o_ref[...] = d if h_ref is None else h_ref[...] + d

        @pl.when(i > 0)
        def _():
            o_ref[...] += d
    return put


def setter(o_ref):
    def put(i, s, d):
        o_ref[:, s] = gelu(d).astype(BF)
    return put


def lamb_a(p, wi, mi, vi, gi, w1, m1, v1, s1, n1, ci, c1, x_ref, wio, mio, vio, w1o, m1o, v1o, h_ref, s_ref, hb, *bufs):
    nbuf = bufs[0].shape[0]
    start, run, drain = lamb_stage('in', 'all', p, wi.shape[0] // 256, wi, mi, vi, (gi,), ci, (wio, mio, vio), bufs[:5],
                                   lambda s: x_ref[:, s], adder(h_ref))
    start2, run2, drain2 = lamb_stage('cols', 'near', p, 4, w1, m1, v1, (s1, n1), c1, (w1o, m1o, v1o), bufs[5:],
                                      lambda s: hb[...], setter(s_ref))
    for i in range(nbuf):
        start(jnp.int32(i))
    run(start2)
    hb[...] = h_ref[...].astype(BF)
    run2()
    drain()
    drain2()


def lamb_b(p, w1, m1, v1, g1, w2, m2, v2, s2, n2, pw, pm, pv, c1, c2, h0_ref, s0_ref,
           w1o, m1o, v1o, w2o, m2o, v2o, s_ref, h_ref, hb, *bufs):
    nbuf = bufs[0].shape[0]
    start, run, drain = lamb_stage('cols', 'far', p, w1.shape[1] // 256 - 4, w1, m1, v1, (g1,), c1, (w1o, m1o, v1o), bufs[:5],
                                   lambda s: hb[...], setter(s_ref))
    start2, run2, drain2 = lamb_stage('out', 'near', p, 4, w2, m2, v2, (s2, n2), c2, (w2o, m2o, v2o), bufs[5:],
                                      lambda s: s_ref[:, s], adder(h_ref, h0_ref))
    for i in range(nbuf):
        start(jnp.int32(i))
    s_ref[...] = s0_ref[...]
    hb[...] = h0_ref[...].astype(BF)
    run(start2)
    run2()
    drain()
    drain2()


def lamb_c(half, p, w2, m2, v2, g2, pw, pm, pv, c2, s_ref, h0_ref, *refs):
    y_ref, refs = (refs[0], refs[1:]) if half == 1 else (None, refs)
    w2o, m2o, v2o, h_ref = refs[:4]
    start, run, drain = lamb_stage('out', f'far{half}', p, w2.shape[0] // 512 - 2, w2, m2, v2, (g2,), c2, (w2o, m2o, v2o),
                                   refs[-5:], lambda s: s_ref[:, s], adder(h_ref, h0_ref))
    for i in range(refs[-5].shape[0]):
        start(jnp.int32(i))
    run()
    if half == 1:
        e = h_ref[...] - y_ref[...].astype(F32)
        row = jnp.sum(e * e, axis=-1, keepdims=True) / (2.0 * e.shape[1])
        refs[4][...] = jnp.broadcast_to(row, (e.shape[0], 128)).T[0:8]
    drain()


def lamb_call(body, name, p, n_hbm, out_hbm, out_vm, kinds, nbuf, blocks, alias, *ins):
    hbm = pl.BlockSpec(memory_space=pltpu.HBM)
    vm = pl.BlockSpec(memory_space=pltpu.VMEM)
    tok = ins[-1].shape[0]
    scratch = [pltpu.VMEM((tok, 1024), BF)] if len(kinds) > 1 else []
    for k in kinds:
        blk = (1024, 256) if k == 'cols' else (256, 1024)
        scratch += [pltpu.VMEM((nbuf, 3) + blk, F32), pltpu.VMEM((nbuf, 256, 1024), BF), pltpu.VMEM((nbuf, 3) + blk, F32),
                    pltpu.SemaphoreType.DMA((nbuf, 4)), pltpu.SemaphoreType.DMA((nbuf, 3))]
    return pl.pallas_call(
        functools.partial(body, p), name=name,
        in_specs=[hbm] * n_hbm + [vm] * (len(ins) - n_hbm),
        out_specs=[hbm] * len(out_hbm) + [vm] * len(out_vm),
        out_shape=[jax.ShapeDtypeStruct(t.shape, F32) for t in out_hbm] + list(out_vm),
        scratch_shapes=scratch,
        input_output_aliases=alias,
        compiler_params=pltpu.CompilerParams(vmem_limit_bytes=54 * 2 ** 20),
        cost_estimate=pl.CostEstimate(flops=25 * 10 ** 8 * blocks, bytes_accessed=blocks * 26 * 2 ** 18, transcendentals=0),
    )(*ins)


def solution(mesh):
    p = mesh.shape['data']

    def gather(s):
        return lax.all_gather(s, 'data', axis=0, tiled=True)

    def step(wi, w1, w2, mi, vi, m1, v1, m2, v2, x0, y0, x1, y1):
        w1, w2, m1, v1, m2, v2 = (t[0] for t in (w1, w2, m1, v1, m2, v2))
        s2, s1, gi, n2, n1, qa, qb, c = reduce_grads(p, x0, y0, w2, m2, v2, w1, m1, v1, wi, mi, vi)
        g1 = gather(s1)
        ga = gather(qa)
        gb = gather(qb)
        tok, d = y0.shape
        hs = jax.ShapeDtypeStruct((tok, d), F32)
        ss = jax.ShapeDtypeStruct((tok, w1.shape[1]), BF)
        ls = jax.ShapeDtypeStruct((8, tok), F32)
        wi_n, mi_n, vi_n, *u, h, s = lamb_call(
            lamb_a, 'lamb_a', p, 9, (wi, mi, vi, w1, m1, v1), (hs, ss), ('in', 'cols'), 3, 20, {},
            wi, mi, vi, gi, w1, m1, v1, s1, n1, c[1], c[2], x1)
        w1_n, m1_n, v1_n, *u, s, h = lamb_call(
            lamb_b, 'lamb_b', p, 12, (w1, m1, v1, w2, m2, v2), (ss, hs), ('cols', 'out'), 3, 16, {9: 0, 10: 1, 11: 2},
            w1, m1, v1, g1, w2, m2, v2, s2, n2, *u, c[2], c[0], h, s)
        *u, h = lamb_call(
            functools.partial(lamb_c, 0), 'lamb_c', p, 7, (w2, m2, v2), (hs,), ('out',), 4, 6, {4: 0, 5: 1, 6: 2},
            w2, m2, v2, ga, *u, c[0], s, h)
        w2_n, m2_n, v2_n, h, loss = lamb_call(
            functools.partial(lamb_c, 1), 'lamb_d', p, 7, (w2, m2, v2), (hs, ls), ('out',), 4, 6, {4: 0, 5: 1, 6: 2},
            w2, m2, v2, gb, *u, c[0], s, h, y1)
        loss = loss[0]
        return (wi_n, w1_n[None], w2_n[None], mi_n, vi_n, m1_n[None], v1_n[None], m2_n[None], v2_n[None], loss, h)

    w2s = P('rep', None)
    w3s = P('rep', None, None)
    ts = P(('rep', 'data'), None)
    return jax.shard_map(step, mesh=mesh,
                         in_specs=(w2s, w3s, w3s, w2s, w2s, w3s, w3s, w3s, w3s, ts, ts, ts, ts),
                         out_specs=(w2s, w3s, w3s, w2s, w2s, w3s, w3s, w3s, w3s, P(('rep', 'data')), ts),
                         check_vma=False)
```
